128 devices in a mesh: dom: 16 (over x, y), harm: 8 (over z, core).
Axes of the slice: x: 4, y: 4, z: 4, core: 2. Of those that a mesh axis runs over, the one named last changes fastest.
Arguments:
- basis: float32 [20, 2, 256, 32768], P(None, None, 'harm', 'dom'), may hold values from -200 to 200, as said below
- coeffs: float32 [20], replicated, may hold values from -4 to 4
- conductance_tiles: float32 [256, 6, 128, 128], P('dom'), may hold values from -0.21875 to 0.21875
- tile_cols: int32 [256, 6], P('dom'), may hold values from 0 to 31, as said below
- self_cond: float32 [32768], P('dom'), may hold values from 1.5 to 4
- cap: float32 [32768], P('dom'), may hold values from 0.05 to 0.5
- send_nodes: int32 [16, 16, 128], P('dom'), may hold values from 0 to 2047, as said below
- send_count: int32 [16, 16], P('dom'), may hold values from 0 to 128, as said below
- nl_nodes: int32 [16, 512], P('dom'), may hold values from 0 to 2047, as said below
- nl_count: int32 [16], P('dom'), may hold values from 1 to 512, 4096 in all
- op_wave: float32 [512, 8192], P(None, ('dom', 'harm')), may hold values from -1.5 to 1
- nl_gain: float32 [8192], P(('dom', 'harm')), may hold values from 0.1 to 1
Outputs:
- new_vector: float32 [2, 256, 32768], P(None, 'harm', 'dom')
- hess_column: float32 [21], replicated
The draws below stay inside these ranges and needn't reach their ends.
Inputs may be any that keep to these rules, and one draw needn't show every extreme that they name: `send_count`: A partition s lists live nodes only for the partitions 1, 15, 8 and 9 places after it (modulo 16), never for itself, at least 32 for each of those, and exactly 128 for at least one of them. `send_nodes`: distinct local nodes within one list. `tile_cols`: every tile of the ghost part of each partition's extended vector is read by some row tile of that partition. `nl_nodes`: distinct local nodes within a partition. The basis vectors are linearly independent.
All inputs are finite; a program needn't handle non-finite values. No bound on the sum of `nl_count` on one device may be relied on, other than what follows from the above.
Results may differ from the reference program's by a relative error of at most 0.0003.
Values sent between devices are 32-bit elements; how exact they have to be, the bound alone decides.
No kernel may reach another device: no remote copies, remote signals or barrier semaphores. Data moves between devices by JAX's collectives and lax.ppermute only.
A program may use at most 128 MiB of HBM per device.

```python
import math
import jax
import jax.numpy as jnp
import numpy as np
from jax import lax

HARM = 256
BASIS = 20
TILE = 128
TPR = 6
PARTITION_NODES = 2048
PEER_CAP = 128
NL_CAP = 512
NL_MEAN = 256
NODES = 32768
NL_ALL = 8192
N_DOM = 16


def draw_basis(key, part):
    first, second = jax.random.split(jax.random.fold_in(key, 11), 2)
    shape_full = (BASIS, 2, HARM, NODES)
    node_frac = jnp.arange(NODES, dtype=jnp.float32) / NODES
    harm_frac = jnp.arange(HARM, dtype=jnp.float32) / HARM
    amplitude = jnp.sqrt(1.0 + 2.0 * node_frac)[None, None, None, :] * jnp.sqrt(1.0 + 2.0 * harm_frac)[None, None, :, None]
    rough = jnp.clip(jax.random.normal(first, shape_full, jnp.float32), -6.0, 6.0)
    common = jnp.clip(jax.random.normal(second, (1, 2, HARM, NODES), jnp.float32), -6.0, 6.0)
    return (rough + 0.7 * common) * amplitude


def draw_tile_cols(key, part):
    first, second = jax.random.split(jax.random.fold_in(key, 17))
    local_tiles = PARTITION_NODES // TILE
    ghost_tiles = N_DOM * PEER_CAP // TILE
    tile_index = jnp.arange(NODES // TILE, dtype=jnp.int32)
    within = tile_index % local_tiles
    owner = tile_index // local_tiles
    offsets = jax.random.randint(first, (N_DOM,), 0, ghost_tiles)[owner]
    last_col = jax.random.randint(second, (NODES // TILE,), 0, local_tiles)
    columns = [within]
    for index in range(TPR - 2):
        columns.append(local_tiles + ((TPR - 2) * within + index + offsets) % ghost_tiles)
    columns.append(last_col)
    return jnp.stack(columns, axis=1).astype(jnp.int32)


def draw_send_nodes(key, part):
    keys = jax.random.split(jax.random.fold_in(key, 21), N_DOM * N_DOM)
    chosen = jax.vmap(lambda single: jax.random.permutation(single, PARTITION_NODES)[:PEER_CAP])(keys)
    return chosen.reshape(N_DOM, N_DOM, PEER_CAP).astype(jnp.int32)


def draw_send_count(key, part):
    first, second = jax.random.split(jax.random.fold_in(key, 31))
    counts = jax.random.randint(first, (N_DOM, N_DOM), PEER_CAP // 4, PEER_CAP + 1)
    sender = jnp.arange(N_DOM, dtype=jnp.int32)
    offsets = jnp.array([1, N_DOM - 1, N_DOM // 2, N_DOM // 2 + 1], dtype=jnp.int32)
    distance = (sender[None, :] - sender[:, None]) % N_DOM
    near = jnp.any(distance[:, :, None] == offsets[None, None, :], axis=2)
    choose = jax.random.randint(second, (N_DOM,), 0, 2)
    jumps = jnp.where(choose == 0, 1, N_DOM // 2)
    full = distance == jumps[:, None]
    counts = jnp.where(near, counts, 0)
    counts = jnp.where(full, PEER_CAP, counts)
    counts = jnp.where(distance == 0, 0, counts)
    return counts.astype(jnp.int32)


def draw_nl_nodes(key, part):
    keys = jax.random.split(jax.random.fold_in(key, 41), N_DOM)
    chosen = jax.vmap(lambda single: jax.random.permutation(single, PARTITION_NODES)[:NL_CAP])(keys)
    return chosen.astype(jnp.int32)


def steps_of(key, shape, cuts, smallest, largest):
    def one(position, blocks):
        steps = jax.random.uniform(jax.random.fold_in(jax.random.fold_in(key, 6), position), (blocks,), jnp.float32, smallest / len(cuts), largest / len(cuts))
        return jnp.repeat(jnp.exp(steps), shape[position] // blocks).reshape((-1,) + (1,) * (len(shape) - position - 1))

    loudness = one(*cuts[0])
    for cut in cuts[1:]:
        loudness = loudness * one(*cut)
    return loudness


def length_profile(count, total, limit, skew):
    loads = [(1 << 20) // math.isqrt(standing ** skew) + 1 for standing in range(2, count + 1)]
    rest, holding = total - limit - (count - 1), [1] * (count - 1)
    while rest > 0:
        movable = [i for i in range(count - 1) if holding[i] < limit]
        whole, left = sum([loads[i] for i in movable]), rest
        for i in movable:
            more = min(limit - holding[i], max(1, left * loads[i] // whole), rest)
            holding[i] = holding[i] + more
            rest = rest - more
    return np.array([limit] + holding)


def uneven_parts(own_key, count, total, most, lean):
    if count == 2:
        one = jax.random.randint(own_key, (), max(1, total - most), min(most, total - 1) + 1)
        return jnp.stack([one, total - one])
    lengths = jnp.asarray(length_profile(count, total, most, lean), jnp.int32)
    twos = (count - 1) // 2
    source_of, taker = lengths[1:1 + 2 * twos:2], lengths[2:2 + 2 * twos:2]
    room = jnp.minimum(source_of - 1, most - taker)
    shifted = jax.random.randint(jax.random.fold_in(own_key, 1), (twos,), 0, 1 << 20) % (room + 1)
    lengths = lengths.at[1:1 + 2 * twos:2].set(source_of - shifted).at[2:2 + 2 * twos:2].set(taker + shifted)
    return lengths[jax.random.permutation(jax.random.fold_in(own_key, 2), count)]


def gaussian(own_key, shape, width, limit, cuts=(), held_as=jnp.bfloat16):
    result = jax.random.normal(own_key, shape, jnp.float32) * width
    if len(cuts) > 0:
        result = steps_of(own_key, shape, cuts, -0.22, 0.18) * result
    return jnp.clip(result, min=-limit, max=limit).astype(held_as)


def setup_inputs(seed: int = 0) -> dict:
    seeds = jax.random.split(jax.random.key(seed), 13)
    return {
        "basis": draw_basis(jax.random.fold_in(seeds[12], 71), 0),
        "coeffs": gaussian(seeds[1], (BASIS,), 1.0, 4.0, (), jnp.float32),
        "conductance_tiles": gaussian(seeds[2], (NODES // TILE, TPR, TILE, TILE), (TPR * TILE) ** -0.5, 0.21875, ((0, 16),), jnp.float32),
        "tile_cols": draw_tile_cols(jax.random.fold_in(seeds[12], 71), 0),
        "self_cond": jnp.clip(jnp.exp(math.log(4.0) - 0.98082925 * jax.random.uniform(seeds[4], (NODES,), jnp.float32) ** steps_of(seeds[4], (NODES,), ((0, 16),), -0.2, 0.2)), 1.5, 4.0),
        "cap": jnp.clip(jnp.exp(math.log(0.5) - 2.3025851 * jax.random.uniform(seeds[5], (NODES,), jnp.float32) ** steps_of(seeds[5], (NODES,), ((0, 16),), -0.2, 0.2)), 0.05, 0.5),
        "send_nodes": draw_send_nodes(jax.random.fold_in(seeds[12], 71), 0),
        "send_count": draw_send_count(jax.random.fold_in(seeds[12], 71), 0),
        "nl_nodes": draw_nl_nodes(jax.random.fold_in(seeds[12], 71), 0),
        "nl_count": uneven_parts(seeds[9], N_DOM, N_DOM * NL_MEAN, NL_CAP, 2).astype(jnp.int32),
        "op_wave": jnp.clip(-1.5 + 2.5 * jax.random.uniform(seeds[10], (2 * HARM, NL_ALL), jnp.float32) ** steps_of(seeds[10], (2 * HARM, NL_ALL), ((1, 128),), -0.2, 0.2), -1.5, 1.0),
        "nl_gain": jnp.clip(jnp.exp(math.log(1.0) - 2.3025851 * jax.random.uniform(seeds[11], (NL_ALL,), jnp.float32) ** steps_of(seeds[11], (NL_ALL,), ((0, 128),), -0.2, 0.2)), 0.1, 1.0),
    }


epsilon = 1e-06

def tables(harmonic, samples):
    sample_index = jnp.arange(samples, dtype=jnp.int32)
    product = harmonic[None, :] * sample_index[:, None] % samples
    angles = 2.0 * math.pi * product.astype(jnp.float32) / samples
    cosine = jnp.cos(angles)
    sine_part = jnp.sin(angles)
    alternating = 1.0 - 2.0 * (sample_index % 2).astype(jnp.float32)
    is_zero = harmonic == 0
    second = jnp.where(is_zero[None, :], alternating[:, None], sine_part)
    inverse = jnp.stack([cosine, second], axis=1)
    weights = jnp.where(is_zero, 1.0 / samples, 2.0 / samples).astype(jnp.float32)
    forward = jnp.transpose(jnp.stack([cosine * weights[None, :], second * weights[None, :]], axis=1), (1, 2, 0))
    return (inverse, forward)

def solve_gram(gram_matrix, projections):
    factor = jnp.linalg.cholesky(gram_matrix)
    size_count = gram_matrix.shape[0]
    middle = jnp.zeros_like(projections)
    for index in range(size_count):
        middle = middle.at[index].set((projections[index] - jnp.dot(factor[index], middle, precision=lax.Precision.HIGHEST)) / factor[index, index])
    answer = jnp.zeros_like(projections)
    for index in range(size_count - 1, -1, -1):
        answer = answer.at[index].set((middle[index] - jnp.dot(factor[:, index], answer, precision=lax.Precision.HIGHEST)) / factor[index, index])
    return answer

def reference(basis, coeffs, conductance_tiles, tile_cols, self_cond, cap, send_nodes, send_count, nl_nodes, nl_count, op_wave, nl_gain):
    highest_harmonic = lax.Precision.HIGHEST
    count_of_rows = 2 * HARM
    vector = jnp.einsum('b,bpkn->pkn', coeffs, basis, precision=highest_harmonic)
    flattened = vector.reshape(count_of_rows, NODES)
    local_tiles = PARTITION_NODES // TILE
    slot_index = jnp.arange(PEER_CAP, dtype=jnp.int32)
    part_index = jnp.arange(N_DOM, dtype=jnp.int32)

    def one_part(receiver):
        listed = lax.dynamic_index_in_dim(send_nodes, receiver, 1, keepdims=False)
        live_counts = lax.dynamic_index_in_dim(send_count, receiver, 1, keepdims=False)
        active = slot_index[None, :] < live_counts[:, None]
        node_index = (listed + part_index[:, None] * PARTITION_NODES).reshape(-1)
        ghosts = jnp.take(flattened, node_index, axis=1).reshape(count_of_rows, N_DOM, PEER_CAP)
        ghosts = jnp.where(active[None], ghosts, 0.0)
        own_block = lax.dynamic_slice_in_dim(flattened, receiver * PARTITION_NODES, PARTITION_NODES, 1).reshape(count_of_rows, local_tiles, TILE)
        extended = jnp.concatenate([own_block, ghosts.reshape(count_of_rows, -1, TILE)], axis=1)
        columns = lax.dynamic_slice_in_dim(tile_cols, receiver * local_tiles, local_tiles, 0)
        node_conductance = lax.dynamic_slice_in_dim(conductance_tiles, receiver * local_tiles, local_tiles, 0)
        picked_entries = jnp.take(extended, columns, axis=1)
        return jnp.einsum('rhfq,hfqo->rho', picked_entries, node_conductance, precision=highest_harmonic).reshape(count_of_rows, PARTITION_NODES)
    coupled_nodes = lax.map(one_part, part_index)
    coupled_nodes = jnp.transpose(coupled_nodes, (1, 0, 2)).reshape(2, HARM, NODES)
    harmonic = jnp.arange(HARM, dtype=jnp.int32)
    angular = 2.0 * math.pi * harmonic.astype(jnp.float32) / HARM
    frequency = jnp.stack([-angular[:, None] * cap[None, :] * vector[1], angular[:, None] * cap[None, :] * vector[0]])
    base = coupled_nodes + self_cond[None, None, :] * vector + frequency
    nl_index = (nl_nodes + part_index[:, None] * PARTITION_NODES).reshape(-1)
    nl_active = (jnp.arange(NL_CAP, dtype=jnp.int32)[None, :] < nl_count[:, None]).reshape(-1)
    sampled = jnp.where(nl_active[None, :], jnp.take(flattened, nl_index, axis=1), 0.0)
    inverse, forward = tables(harmonic, count_of_rows)
    waveform = jnp.dot(inverse.reshape(count_of_rows, count_of_rows), sampled, precision=highest_harmonic)
    current = nl_gain[None, :] * jnp.exp(op_wave) * waveform
    returned = jnp.dot(forward.reshape(count_of_rows, count_of_rows), current, precision=highest_harmonic)
    returned = jnp.where(nl_active[None, :], returned, 0.0)
    product = base.reshape(count_of_rows, NODES).at[:, nl_index].add(returned).reshape(2, HARM, NODES)
    entries = 2 * HARM * NODES
    gram_matrix = jnp.einsum('apkn,bpkn->ab', basis, basis, precision=highest_harmonic) / entries
    projections = jnp.einsum('apkn,pkn->a', basis, product, precision=highest_harmonic) / entries
    hess = solve_gram(gram_matrix, projections)
    residual = product - jnp.einsum('a,apkn->pkn', hess, basis, precision=highest_harmonic)
    mean_square = jnp.sum(residual * residual) / entries
    norm_value = jnp.sqrt(mean_square + epsilon)
    return (residual / norm_value, jnp.concatenate([hess, norm_value[None]]))
```

```python
import functools
import math

import ml_dtypes
import numpy as np

import jax
import jax.numpy as jnp
from jax import lax
from jax.experimental import pallas as pl
from jax.experimental.pallas import tpu as pltpu
from jax.sharding import Mesh
from jax.sharding import PartitionSpec as P

HARM = 256
SAMPLES = 2 * HARM
DOM = ("dom_0", "dom_1")
HARM_AXES = ("harm_0", "harm_1")
DOM_HARM = ("dom_0", "dom_1", "harm_0", "harm_1")
PEERS = (1, 15, 8, 9)
EPSILON = 1e-06

F32 = jnp.float32
BF16 = jnp.bfloat16


def halves(value):
    high = value.astype(BF16)
    return high, (value - high.astype(F32)).astype(BF16)


def thirds(value):
    high = value.astype(BF16)
    rest = value - high.astype(F32)
    middle = rest.astype(BF16)
    return high, middle, (rest - middle.astype(F32)).astype(BF16)


def mm(left, right):
    return jnp.dot(left, right, preferred_element_type=F32)


def mm_nt(left, right):
    return lax.dot_general(left, right, (((1,), (1,)), ((), ())), preferred_element_type=F32)


def split_table(table):
    high = table.astype(ml_dtypes.bfloat16)
    low = (table - high.astype(np.float64)).astype(ml_dtypes.bfloat16)
    return [high, low]


def transform_tables():
    index = np.arange(HARM)
    angle = 2.0 * np.pi * ((index[:, None] * index[None, :]) % SAMPLES) / SAMPLES
    cosine, sine = np.cos(angle), np.sin(angle)
    sine[:, 0] = 1.0 - 2.0 * (index % 2)
    return np.stack(split_table(cosine) + split_table(sine) + split_table(sine.T))


def pair_list(count):
    return [(i, j) for i in range(count) for j in range(i, count)]


def unpack_tables(count, rows, width):
    pairs = pair_list(count)
    mask = np.zeros((2, rows, width), np.float32)
    place = np.zeros((2, width, 128), np.float32)
    for position, (i, j) in enumerate(pairs):
        mask[0, i, position] = 1.0
        place[0, position, j] = 1.0
        if i != j:
            mask[1, j, position] = 1.0
            place[1, position, i] = 1.0
    for i in range(count):
        mask[0, i, len(pairs) + i] = 1.0
        place[0, len(pairs) + i, count] = 1.0
    return mask, place.astype(ml_dtypes.bfloat16)


def basis_copy(source, target, sems, block):
    rows = pl.ds(pl.multiple_of(block * 8, 8), 8)
    return pltpu.make_async_copy(source.at[:, rows, :], target.at[:, rows, :], sems.at[block])


def start_all(source, target, sems):
    for block in range(target.shape[1] // 8):
        basis_copy(source, target, sems, block).start()


def row_total(rows_ref):
    ones = jnp.ones((8, rows_ref.shape[1]), BF16)
    return sum(mm_nt(ones, part) for part in thirds(rows_ref[...]))


def vector_kernel(coeffs, send_count, nl_count, send_nodes, nl_nodes, basis_hbm,
                  vector, ghost_0, ghost_1, ghost_2, ghost_3, sampled,
                  basis, select, sems):
    start_all(basis_hbm, basis, sems)
    count, rows, nodes = basis.shape
    peers = send_nodes.shape[0]
    slots = nl_nodes.shape[1]
    cap = send_nodes.shape[1]
    me = lax.axis_index(DOM)
    lane = lax.broadcasted_iota(jnp.int32, (1, cap), 1)
    wanted = []
    for step in PEERS:
        peer = lax.rem(me + step, peers)
        listed = send_nodes[pl.ds(peer, 1), :]
        wanted.append(jnp.where(lane < send_count[peer], listed, -1))
    slot = lax.broadcasted_iota(jnp.int32, (1, slots), 1)
    wanted.append(jnp.where(slot < nl_count[0], nl_nodes[...], -1))
    columns = jnp.concatenate(wanted, axis=1)
    chunk = nodes // (rows // 8)

    @pl.loop(0, rows // 8)
    def _(block):
        start = pl.multiple_of(block * chunk, chunk)
        node = lax.broadcasted_iota(jnp.int32, (chunk, columns.shape[1]), 0) + start
        select[pl.ds(start, chunk), :] = jnp.where(node == columns, 1.0, 0.0).astype(BF16)
        basis_copy(basis_hbm, basis, sems, block).wait()
        part = pl.ds(pl.multiple_of(block * 8, 8), 8)
        total = coeffs[0] * basis[0, part, :]
        for j in range(1, count):
            total = total + coeffs[j] * basis[j, part, :]
        vector[part, :] = total

    left = jnp.concatenate(halves(vector[...]), axis=0)
    for peer, ghost in enumerate((ghost_0, ghost_1, ghost_2, ghost_3)):
        taken = mm(left, select[:, peer * cap : (peer + 1) * cap])
        ghost[...] = taken[:rows] + taken[rows:]
    half = rows // 2
    low_lanes = lax.broadcasted_iota(jnp.int32, (half, 128), 1) < 64
    for pair in range(slots // 128):
        first = len(PEERS) * cap + pair * 128
        taken = mm(left, select[:, first : first + 128])
        taken = taken[:rows] + taken[rows:]
        top, bottom = taken[:half], taken[half:]
        sampled[2 * pair] = jnp.where(low_lanes, top, pltpu.roll(bottom, 64, 1))
        sampled[2 * pair + 1] = jnp.where(low_lanes, pltpu.roll(top, 64, 1), bottom)


def gram_kernel(basis_hbm, packed, basis, sums, totals, sems):
    start_all(basis_hbm, basis, sems)
    count, rows, nodes = basis.shape
    position = {pair: p for p, pair in enumerate(pair_list(count))}
    group = 5
    groups = [range(g, g + group) for g in range(0, count, group)]
    sums[...] = jnp.zeros_like(sums)

    @pl.loop(0, rows // 8)
    def _(block):
        basis_copy(basis_hbm, basis, sems, block).wait()
        part = pl.ds(pl.multiple_of(block * 8, 8), 8)
        for x, left in enumerate(groups):
            for right in groups[x:]:
                names = [(i, j) for i in left for j in right if i <= j]
                held = {}
                for chunk in range(nodes // 128):
                    lanes = slice(chunk * 128, (chunk + 1) * 128)
                    value = {i: basis[i, part, lanes] for i in set(left) | set(right)}
                    for i, j in names:
                        term = value[i] * value[j]
                        held[i, j] = held[i, j] + term if chunk else term
                for pair in names:
                    sums[position[pair]] += held[pair]

    totals[...] = jnp.zeros_like(totals)
    for p in range(len(position)):
        totals[p : p + 1, :] = jnp.sum(sums[p], axis=0, keepdims=True)
    packed[...] = row_total(totals)


def current_kernel(arrived, wave, gain, tables, leaving):
    half = HARM // 2
    spectrum = arrived[...].reshape(HARM, 128)
    lane = lax.broadcasted_iota(jnp.int32, (HARM, 128), 1)
    harmonic = lax.broadcasted_iota(jnp.int32, (HARM, 128), 0)
    low = lane < 64
    sign = jnp.where(harmonic % 2 == 0, 1.0, -1.0)
    swapped = pltpu.roll(spectrum, 64, 1)
    even = jnp.where(low, spectrum, swapped * sign)
    odd = jnp.where(low, swapped, spectrum * sign)

    def product(index, values):
        high, lower = values
        return (
            mm(tables[index], high) + mm(tables[index], lower) + mm(tables[index + 1], high)
        )

    waveform = product(0, halves(even)) + product(2, halves(odd))
    gains = jnp.concatenate([gain[...], gain[...]], axis=1)
    growth = jnp.exp(jnp.concatenate([wave[:HARM], wave[HARM:]], axis=1))
    current = halves(gains * growth * waveform)
    weight = jnp.where(harmonic == 0, 1.0 / SAMPLES, 2.0 / SAMPLES)
    cosine = product(0, current)
    sine = product(4, current)
    result = weight * jnp.where(
        low,
        cosine + sign * pltpu.roll(cosine, 64, 1),
        sign * sine + pltpu.roll(sine, 64, 1),
    )
    leaving[...] = result.reshape(leaving.shape)


def coupling_kernel(tile_cols, vector, ghost_0, ghost_1, ghost_2, ghost_3,
                    self_cond, cap, tiles, base, extended):
    rows, nodes = vector.shape
    half = rows // 2
    local_tiles = nodes // 128
    peers = extended.shape[0] - local_tiles
    step = pl.program_id(0)
    me = lax.axis_index(DOM)

    @pl.when(step == 0)
    def _():
        for tile in range(local_tiles):
            high, low = halves(vector[:, tile * 128 : (tile + 1) * 128])
            extended[tile, :rows] = high
            extended[tile, rows:] = low
        extended[local_tiles:] = jnp.zeros((peers, 2 * rows, 128), BF16)
        for jump, ghost in zip(PEERS, (ghost_0, ghost_1, ghost_2, ghost_3)):
            sender = local_tiles + lax.rem(me + peers - jump, peers)
            high, low = halves(ghost[...])
            extended[sender, :rows] = high
            extended[sender, rows:] = low

    per_step, terms = tiles.shape[0], tiles.shape[1]
    first = lax.axis_index(HARM_AXES) * half
    harmonic = first + lax.broadcasted_iota(jnp.int32, (half, 128), 0)
    angular = (2.0 * math.pi / HARM) * harmonic.astype(F32)
    for t in range(per_step):
        row = step * per_step + t
        total = jnp.zeros((rows, 128), F32)
        for i in range(0, terms, 2):
            left = jnp.concatenate(
                [extended[tile_cols[row, i]], extended[tile_cols[row, i + 1]]], axis=1
            )
            high, low = halves(tiles[t, i : i + 2].reshape(256, 128))
            main = mm(left, high)
            total = total + main[:rows] + main[rows:] + mm(left[:rows], low)
        lanes = pl.ds(pl.multiple_of(row * 128, 128), 128)
        cosine, sine = vector[:half, lanes], vector[half:, lanes]
        ground, reactive = self_cond[:, lanes], angular * cap[:, lanes]
        base[:half, lanes] = total[:half] + ground * cosine - reactive * sine
        base[half:, lanes] = total[half:] + ground * sine + reactive * cosine


def product_kernel(nl_count, nl_nodes, arrived, base, packed_gram, basis_hbm,
                   product, packed, basis, totals, sems):
    start_all(basis_hbm, basis, sems)
    count, rows, nodes = basis.shape
    half = rows // 2
    slots = nl_nodes.shape[1]
    slot = lax.broadcasted_iota(jnp.int32, (1, slots), 1)
    columns = jnp.where(slot < nl_count[0], nl_nodes[...], -1)
    low_lanes = lax.broadcasted_iota(jnp.int32, (half, 128), 1) < 64
    top, bottom = [], []
    for pair in range(slots // 128):
        even, odd = arrived[2 * pair], arrived[2 * pair + 1]
        top.append(jnp.where(low_lanes, even, pltpu.roll(odd, 64, 1)))
        bottom.append(jnp.where(low_lanes, pltpu.roll(even, 64, 1), odd))
    returned = jnp.concatenate(
        [jnp.concatenate(top, axis=1), jnp.concatenate(bottom, axis=1)], axis=0
    )
    left = jnp.concatenate(halves(returned), axis=0)
    width = 256
    for start in range(0, nodes, width):
        node = lax.broadcasted_iota(jnp.int32, (width, slots), 0) + start
        chosen = jnp.where(node == columns, 1.0, 0.0).astype(BF16)
        added = mm_nt(left, chosen)
        lanes = slice(start, start + width)
        product[:, lanes] = base[:, lanes] + added[:rows] + added[rows:]

    def block_sums(block, sums):
        basis_copy(basis_hbm, basis, sems, block).wait()
        part = pl.ds(pl.multiple_of(block * 8, 8), 8)
        sums = list(sums)
        for chunk in range(nodes // 128):
            lanes = slice(chunk * 128, (chunk + 1) * 128)
            value = product[part, lanes]
            for a in range(count):
                sums[a] = sums[a] + basis[a, part, lanes] * value
            sums[count] = sums[count] + value * value
        return tuple(sums)

    sums = lax.fori_loop(
        0, rows // 8, block_sums, tuple(jnp.zeros((8, 128), F32) for _ in range(count + 1))
    )
    totals[...] = jnp.zeros_like(totals)
    first = count * (count + 1) // 2
    for a in range(count + 1):
        totals[first + a : first + a + 1, :] = jnp.sum(sums[a], axis=0, keepdims=True)
    line = (row_total(totals) + packed_gram[...])[:1]
    both = jnp.concatenate([line[:, :128], line[:, 128:]], axis=0)
    packed[...] = jnp.broadcast_to(both[None], packed.shape)


def residual_kernel(entries, gathered, mask, place, product, basis_hbm,
                    residual, column, basis, weights, sems):
    start_all(basis_hbm, basis, sems)
    count, rows, nodes = basis.shape
    height = mask.shape[1]
    scale = 1.0 / entries
    summed = jnp.sum(gathered[...], axis=0) * scale
    line = jnp.concatenate([summed[:1], summed[1:]], axis=1)
    system = jnp.zeros((height, 128), F32)
    for side in range(2):
        spread = mask[side] * line
        for part in thirds(spread):
            system = system + mm(part, place[side])
    lane = lax.broadcasted_iota(jnp.int32, (height, 128), 1)
    row = lax.broadcasted_iota(jnp.int32, (height, 128), 0)
    proj = jnp.sum(jnp.where(lane == count, system, 0.0), axis=1, keepdims=True)
    work = system
    for k in range(count):
        pivot_row = work[k : k + 1, :]
        pivot = pivot_row[:, k : k + 1]
        scaled = pivot_row / pivot
        work = jnp.where(row == k, scaled, work - work[:, k : k + 1] * scaled)
    solved = work[:, count : count + 1]
    solved = jnp.where(row[:, :1] < count, solved, 0.0)
    first = count * (count + 1) // 2
    energy = line[:, first + count : first + count + 1]
    mean_square = energy - jnp.sum(proj * solved, axis=0, keepdims=True)
    norm = jnp.sqrt(mean_square + EPSILON)
    wide = jnp.broadcast_to(solved, (height, 128))
    as_row = jnp.sum(jnp.where(lane == row, wide, 0.0), axis=0, keepdims=True)
    as_row = jnp.where(lane[:1] == count, norm, as_row)
    column[...] = as_row[:, : count + 1]
    weights[...] = wide
    inverse = jnp.broadcast_to(1.0 / norm, (8, 128))

    @pl.loop(0, rows // 8)
    def _(block):
        basis_copy(basis_hbm, basis, sems, block).wait()
        part = pl.ds(pl.multiple_of(block * 8, 8), 8)
        hess = [jnp.broadcast_to(weights[a : a + 1, :], (8, 128)) for a in range(count)]
        for chunk in range(nodes // 128):
            lanes = slice(chunk * 128, (chunk + 1) * 128)
            terms = [hess[a] * basis[a, part, lanes] for a in range(count)]
            while len(terms) > 1:
                terms = [sum(terms[i : i + 2]) for i in range(0, len(terms), 2)]
            residual[part, lanes] = (product[part, lanes] - terms[0]) * inverse


def local(
    basis,
    coeffs,
    conductance_tiles,
    tile_cols,
    self_cond,
    cap,
    send_nodes,
    send_count,
    nl_nodes,
    nl_count,
    op_wave,
    nl_gain,
):
    count, _, harm_local, nodes = basis.shape
    rows = 2 * harm_local
    peers = lax.axis_size(DOM)
    groups = lax.axis_size(HARM_AXES)
    peer_cap = send_nodes.shape[2]
    nl_cap = nl_nodes.shape[1]
    basis = basis.reshape(count, rows, nodes)
    smem = pl.BlockSpec(memory_space=pltpu.SMEM)
    vmem = pl.BlockSpec(memory_space=pltpu.VMEM)
    hbm = pl.BlockSpec(memory_space=pl.ANY)
    shape = jax.ShapeDtypeStruct
    basis_scratch = pltpu.VMEM((count, rows, nodes), F32)
    sems = pltpu.SemaphoreType.DMA((rows // 8,))
    basis_bytes = 4 * count * rows * nodes

    def cost(flops, size):
        return pl.CostEstimate(flops=flops, bytes_accessed=size, transcendentals=0)

    vector, *ghosts, sampled = pl.pallas_call(
        vector_kernel,
        out_shape=[shape((rows, nodes), F32)]
        + [shape((rows, peer_cap), F32)] * len(PEERS)
        + [shape((groups, harm_local, 128), F32)],
        in_specs=[smem, smem, smem, vmem, vmem, hbm],
        out_specs=[vmem] * (2 + len(PEERS)),
        scratch_shapes=[
            basis_scratch,
            pltpu.VMEM((nodes, len(PEERS) * peer_cap + nl_cap), BF16),
            sems,
        ],
        cost_estimate=cost(10**9, basis_bytes),
        name="vector",
    )(coeffs, send_count[0], nl_count, send_nodes[0], nl_nodes, basis)

    arrived_spectrum = lax.all_to_all(sampled, HARM_AXES, 0, 0, tiled=True)
    ghosts = [
        lax.ppermute(ghost, DOM, [(i, (i + jump) % peers) for i in range(peers)])
        for jump, ghost in zip(PEERS, ghosts)
    ]

    width = 256
    packed_gram = pl.pallas_call(
        gram_kernel,
        out_shape=shape((8, width), F32),
        in_specs=[hbm],
        out_specs=vmem,
        scratch_shapes=[
            basis_scratch,
            pltpu.VMEM((count * (count + 1) // 2, 8, 128), F32),
            pltpu.VMEM((width, 128), F32),
            sems,
        ],
        cost_estimate=cost(10**9, basis_bytes),
        name="gram",
    )(basis)

    leaving = pl.pallas_call(
        current_kernel,
        out_shape=shape((groups, harm_local, 128), F32),
        in_specs=[vmem] * 4,
        out_specs=vmem,
        cost_estimate=cost(4 * 10**8, 2 * 10**6),
        name="current",
    )(arrived_spectrum, op_wave, nl_gain.reshape(1, -1), jnp.asarray(transform_tables()))

    returned = lax.all_to_all(leaving, HARM_AXES, 0, 0, tiled=True)

    tile_rows, terms = tile_cols.shape
    per_step = 2
    whole = lambda *dims: pl.BlockSpec(dims, lambda i: (0,) * len(dims))
    base = pl.pallas_call(
        coupling_kernel,
        grid=(tile_rows // per_step,),
        out_shape=shape((rows, nodes), F32),
        in_specs=[smem, whole(rows, nodes)]
        + [whole(rows, peer_cap)] * len(PEERS)
        + [
            whole(1, nodes),
            whole(1, nodes),
            pl.BlockSpec((per_step, terms, 128, 128), lambda i: (i, 0, 0, 0)),
        ],
        out_specs=whole(rows, nodes),
        scratch_shapes=[pltpu.VMEM((nodes // 128 + peers, 2 * rows, 128), BF16)],
        cost_estimate=cost(10**9, 4 * tile_rows * terms * 128 * 128),
        name="coupling",
    )(
        tile_cols, vector, *ghosts, self_cond.reshape(1, -1), cap.reshape(1, -1),
        conductance_tiles,
    )

    devices = peers * groups
    product, packed = pl.pallas_call(
        product_kernel,
        out_shape=[shape((rows, nodes), F32), shape((devices, width // 128, 128), F32)],
        in_specs=[smem, vmem, vmem, vmem, vmem, hbm],
        out_specs=[vmem, vmem],
        scratch_shapes=[
            basis_scratch,
            pltpu.VMEM((width, 128), F32),
            sems,
        ],
        cost_estimate=cost(10**9, basis_bytes),
        name="product",
    )(nl_count, nl_nodes, returned, base, packed_gram, basis)

    gathered = lax.all_to_all(packed, DOM_HARM, 0, 0, tiled=True)

    entries = rows * groups * nodes * peers
    mask, place = unpack_tables(count, 24, width)
    residual, column = pl.pallas_call(
        functools.partial(residual_kernel, float(entries)),
        out_shape=[shape((rows, nodes), F32), shape((1, count + 1), F32)],
        in_specs=[vmem, vmem, vmem, vmem, hbm],
        out_specs=[vmem, vmem],
        scratch_shapes=[basis_scratch, pltpu.VMEM((24, 128), F32), sems],
        cost_estimate=cost(10**9, basis_bytes),
        name="residual",
    )(gathered, jnp.asarray(mask), jnp.asarray(place), product, basis)
    return (residual.reshape(2, harm_local, nodes), column.reshape(count + 1))


def solution(mesh):
    split = Mesh(mesh.devices.reshape(4, 4, 4, 2), ("dom_0", "dom_1", "harm_0", "harm_1"))
    return jax.shard_map(
        local,
        mesh=split,
        in_specs=(
            P(None, None, HARM_AXES, DOM),
            P(),
            P(DOM, None, None, None),
            P(DOM, None),
            P(DOM),
            P(DOM),
            P(DOM, None, None),
            P(DOM, None),
            P(DOM, None),
            P(DOM),
            P(None, DOM_HARM),
            P(DOM_HARM),
        ),
        out_specs=(P(None, HARM_AXES, DOM), P()),
        check_vma=False,
    )
```

```python
import functools
import math

import ml_dtypes
import numpy as np

import jax
import jax.numpy as jnp
from jax import lax
from jax.experimental import pallas as pl
from jax.experimental.pallas import tpu as pltpu
from jax.sharding import Mesh
from jax.sharding import PartitionSpec as P

HARM = 256
SAMPLES = 2 * HARM
DOM = ("dom_0", "dom_1")
HARM_AXES = ("harm_0", "harm_1")
DOM_HARM = ("dom_0", "dom_1", "harm_0", "harm_1")
PEERS = (1, 15, 8, 9)
EPSILON = 1e-06

F32 = jnp.float32
BF16 = jnp.bfloat16


def halves(value):
    high = value.astype(BF16)
    return high, (value - high.astype(F32)).astype(BF16)


def thirds(value):
    high = value.astype(BF16)
    rest = value - high.astype(F32)
    middle = rest.astype(BF16)
    return high, middle, (rest - middle.astype(F32)).astype(BF16)


def mm(left, right):
    return jnp.dot(left, right, preferred_element_type=F32)


def mm_nt(left, right):
    return lax.dot_general(left, right, (((1,), (1,)), ((), ())), preferred_element_type=F32)


def split_table(table):
    high = table.astype(ml_dtypes.bfloat16)
    low = (table - high.astype(np.float64)).astype(ml_dtypes.bfloat16)
    return [high, low]


def transform_tables():
    index = np.arange(HARM)
    angle = 2.0 * np.pi * ((index[:, None] * index[None, :]) % SAMPLES) / SAMPLES
    cosine, sine = np.cos(angle), np.sin(angle)
    sine[:, 0] = 1.0 - 2.0 * (index % 2)
    return np.stack(split_table(cosine) + split_table(sine) + split_table(sine.T))


def pair_list(count):
    return [(i, j) for i in range(count) for j in range(i, count)]


def unpack_tables(count, rows, width):
    pairs = pair_list(count)
    mask = np.zeros((2, rows, width), np.float32)
    place = np.zeros((2, width, 128), np.float32)
    for position, (i, j) in enumerate(pairs):
        mask[0, i, position] = 1.0
        place[0, position, j] = 1.0
        if i != j:
            mask[1, j, position] = 1.0
            place[1, position, i] = 1.0
    for i in range(count):
        mask[0, i, len(pairs) + i] = 1.0
        place[0, len(pairs) + i, count] = 1.0
    return mask, place.astype(ml_dtypes.bfloat16)


def basis_copy(source, target, sems, block):
    rows = pl.ds(pl.multiple_of(block * 8, 8), 8)
    return pltpu.make_async_copy(source.at[:, rows, :], target.at[:, rows, :], sems.at[block])


def start_all(source, target, sems):
    for block in range(target.shape[1] // 8):
        basis_copy(source, target, sems, block).start()


def row_total(rows_ref):
    ones = jnp.ones((8, rows_ref.shape[1]), BF16)
    return sum(mm_nt(ones, part) for part in thirds(rows_ref[...]))


def vector_kernel(coeffs, send_count, nl_count, send_nodes, nl_nodes, basis_hbm,
                  vector, ghost_0, ghost_1, ghost_2, ghost_3, sampled, cross,
                  basis, select, sems):
    start_all(basis_hbm, basis, sems)
    count, rows, nodes = basis.shape
    peers = send_nodes.shape[0]
    slots = nl_nodes.shape[1]
    cap = send_nodes.shape[1]
    me = lax.axis_index(DOM)
    lane = lax.broadcasted_iota(jnp.int32, (1, cap), 1)
    wanted = []
    for step in PEERS:
        peer = lax.rem(me + step, peers)
        listed = send_nodes[pl.ds(peer, 1), :]
        wanted.append(jnp.where(lane < send_count[peer], listed, -1))
    slot = lax.broadcasted_iota(jnp.int32, (1, slots), 1)
    wanted.append(jnp.where(slot < nl_count[0], nl_nodes[...], -1))
    columns = jnp.concatenate(wanted, axis=1)
    chunk = nodes // (rows // 8)
    cross[...] = jnp.zeros_like(cross)

    @pl.loop(0, rows // 8)
    def _(block):
        start = pl.multiple_of(block * chunk, chunk)
        node = lax.broadcasted_iota(jnp.int32, (chunk, columns.shape[1]), 0) + start
        select[pl.ds(start, chunk), :] = jnp.where(node == columns, 1.0, 0.0).astype(BF16)
        basis_copy(basis_hbm, basis, sems, block).wait()
        part = pl.ds(pl.multiple_of(block * 8, 8), 8)
        total = coeffs[0] * basis[0, part, :]
        for j in range(1, count):
            total = total + coeffs[j] * basis[j, part, :]
        vector[part, :] = total
        both = halves(basis[:, part, :].reshape(count * 8, nodes))
        cross[...] += mm_nt(jnp.concatenate(both, axis=0), both[0])

    left = jnp.concatenate(halves(vector[...]), axis=0)
    half = rows // 2
    low_lanes = lax.broadcasted_iota(jnp.int32, (half, 128), 1) < 64
    ghosts = (ghost_0, ghost_1, ghost_2, ghost_3)
    for start in range(0, columns.shape[1], 256):
        both = mm(left, select[:, start : start + 256])
        both = both[:rows] + both[rows:]
        for item, taken in enumerate((both[:, :128], both[:, 128:])):
            item += start // 128
            if item < len(PEERS):
                ghosts[item][...] = taken
                continue
            pair = item - len(PEERS)
            top, bottom = taken[:half], taken[half:]
            sampled[2 * pair] = jnp.where(low_lanes, top, pltpu.roll(bottom, 64, 1))
            sampled[2 * pair + 1] = jnp.where(low_lanes, pltpu.roll(top, 64, 1), bottom)


def gram_line(cross, mask, place):
    size = cross.shape[1]
    row = lax.broadcasted_iota(jnp.int32, (size, size), 0)
    column = lax.broadcasted_iota(jnp.int32, (size, size), 1)
    matching = row % 8 == column % 8
    first = jnp.where(matching, cross[:size] + cross[size:], 0.0)
    second = jnp.where(matching, cross[size:], 0.0)
    vector = lax.broadcasted_iota(jnp.int32, (128, size), 0)
    owner = lax.broadcasted_iota(jnp.int32, (128, size), 1) // 8
    select = jnp.where(vector == owner, 1.0, 0.0).astype(BF16)
    first = sum(mm(select, part) for part in thirds(first))
    second = sum(mm(select, part) for part in thirds(second))
    gram = sum(mm_nt(part, select) for part in thirds(first))
    gram = gram + sum(mm_nt(select, part) for part in thirds(second))
    height = mask.shape[1]
    spread = sum(mm_nt(part, place[0]) for part in thirds(gram[:height]))
    return jnp.sum(mask[0] * spread, axis=0, keepdims=True)


def current_kernel(arrived, wave, gain, tables, leaving):
    half = HARM // 2
    spectrum = arrived[...].reshape(HARM, 128)
    lane = lax.broadcasted_iota(jnp.int32, (HARM, 128), 1)
    harmonic = lax.broadcasted_iota(jnp.int32, (HARM, 128), 0)
    low = lane < 64
    sign = jnp.where(harmonic % 2 == 0, 1.0, -1.0)
    swapped = pltpu.roll(spectrum, 64, 1)
    even = jnp.where(low, spectrum, swapped * sign)
    odd = jnp.where(low, swapped, spectrum * sign)

    def product(index, values):
        high, lower = values
        return (
            mm(tables[index], high) + mm(tables[index], lower) + mm(tables[index + 1], high)
        )

    waveform = product(0, halves(even)) + product(2, halves(odd))
    gains = jnp.concatenate([gain[...], gain[...]], axis=1)
    growth = jnp.exp(jnp.concatenate([wave[:, :HARM], wave[:, HARM:]], axis=0).T)
    current = halves(gains * growth * waveform)
    weight = jnp.where(harmonic == 0, 1.0 / SAMPLES, 2.0 / SAMPLES)
    cosine = product(0, current)
    sine = product(4, current)
    result = weight * jnp.where(
        low,
        cosine + sign * pltpu.roll(cosine, 64, 1),
        sign * sine + pltpu.roll(sine, 64, 1),
    )
    leaving[...] = result.reshape(leaving.shape)


def coupling_kernel(tile_cols, vector, ghost_0, ghost_1, ghost_2, ghost_3,
                    self_cond, cap, tiles_hbm, base, extended, tiles, sems):
    tile_rows, terms = tiles.shape[:2]

    def tile_copy(row):
        return pltpu.make_async_copy(tiles_hbm.at[row], tiles.at[row], sems.at[row])

    for row in range(tile_rows):
        tile_copy(row).start()
    rows, nodes = vector.shape
    half = rows // 2
    local_tiles = nodes // 128
    peers = extended.shape[0] - local_tiles
    me = lax.axis_index(DOM)
    for tile in range(local_tiles):
        high, low = halves(vector[:, tile * 128 : (tile + 1) * 128])
        extended[tile, :rows] = high
        extended[tile, rows:] = low
    extended[local_tiles:] = jnp.zeros((peers, 2 * rows, 128), BF16)
    for jump, ghost in zip(PEERS, (ghost_0, ghost_1, ghost_2, ghost_3)):
        sender = local_tiles + lax.rem(me + peers - jump, peers)
        high, low = halves(ghost[...])
        extended[sender, :rows] = high
        extended[sender, rows:] = low

    first = lax.axis_index(HARM_AXES) * half
    harmonic = first + lax.broadcasted_iota(jnp.int32, (half, 128), 0)
    angular = (2.0 * math.pi / HARM) * harmonic.astype(F32)

    def one_row(row):
        tile_copy(row).wait()
        left = jnp.concatenate([extended[tile_cols[i, row]] for i in range(terms)], axis=1)
        right = jnp.concatenate(halves(tiles[row].reshape(terms * 128, 128)), axis=1)
        total = mm(left, right)
        total = total[:rows, :128] + total[rows:, :128] + total[:rows, 128:]
        lanes = pl.ds(pl.multiple_of(row * 128, 128), 128)
        cosine, sine = vector[:half, lanes], vector[half:, lanes]
        ground, reactive = self_cond[:, lanes], angular * cap[:, lanes]
        base[:half, lanes] = total[:half] + ground * cosine - reactive * sine
        base[half:, lanes] = total[half:] + ground * sine + reactive * cosine

    pl.loop(0, tile_rows)(one_row)


def product_kernel(nl_count, nl_nodes, arrived, base, cross, mask, place, basis_hbm,
                   product, packed, basis, totals, sems):
    start_all(basis_hbm, basis, sems)
    count, rows, nodes = basis.shape
    half = rows // 2
    slots = nl_nodes.shape[1]
    slot = lax.broadcasted_iota(jnp.int32, (1, slots), 1)
    columns = jnp.where(slot < nl_count[0], nl_nodes[...], -1)
    low_lanes = lax.broadcasted_iota(jnp.int32, (half, 128), 1) < 64
    top, bottom = [], []
    for pair in range(slots // 128):
        even, odd = arrived[2 * pair], arrived[2 * pair + 1]
        top.append(jnp.where(low_lanes, even, pltpu.roll(odd, 64, 1)))
        bottom.append(jnp.where(low_lanes, pltpu.roll(even, 64, 1), odd))
    returned = jnp.concatenate(
        [jnp.concatenate(top, axis=1), jnp.concatenate(bottom, axis=1)], axis=0
    )
    left = jnp.concatenate(halves(returned), axis=0)
    width = 256
    for start in range(0, nodes, width):
        node = lax.broadcasted_iota(jnp.int32, (width, slots), 0) + start
        chosen = jnp.where(node == columns, 1.0, 0.0).astype(BF16)
        added = mm_nt(left, chosen)
        lanes = slice(start, start + width)
        product[:, lanes] = base[:, lanes] + added[:rows] + added[rows:]

    def block_sums(block, sums):
        basis_copy(basis_hbm, basis, sems, block).wait()
        part = pl.ds(pl.multiple_of(block * 8, 8), 8)
        sums = list(sums)
        for chunk in range(nodes // 128):
            lanes = slice(chunk * 128, (chunk + 1) * 128)
            value = product[part, lanes]
            for a in range(count):
                sums[a] = sums[a] + basis[a, part, lanes] * value
            sums[count] = sums[count] + value * value
        return tuple(sums)

    sums = lax.fori_loop(
        0, rows // 8, block_sums, tuple(jnp.zeros((8, 128), F32) for _ in range(count + 1))
    )
    totals[...] = jnp.zeros_like(totals)
    first = count * (count + 1) // 2
    for a in range(count + 1):
        totals[first + a : first + a + 1, :] = jnp.sum(sums[a], axis=0, keepdims=True)
    line = row_total(totals)[:1] + gram_line(cross, mask, place)
    both = jnp.concatenate([line[:, :128], line[:, 128:]], axis=0)
    packed[...] = jnp.broadcast_to(both[None], packed.shape)


def residual_kernel(entries, gathered, mask, place, product, basis,
                    residual, column, weights):
    count, rows, nodes = basis.shape
    height = mask.shape[1]
    scale = 1.0 / entries
    summed = jnp.sum(gathered[...], axis=0) * scale
    line = jnp.concatenate([summed[:1], summed[1:]], axis=1)
    system = jnp.zeros((height, 128), F32)
    for side in range(2):
        spread = mask[side] * line
        for part in thirds(spread):
            system = system + mm(part, place[side])
    lane = lax.broadcasted_iota(jnp.int32, (height, 128), 1)
    row = lax.broadcasted_iota(jnp.int32, (height, 128), 0)
    proj = jnp.sum(jnp.where(lane == count, system, 0.0), axis=1, keepdims=True)
    work = system
    for k in range(count):
        pivot_row = work[k : k + 1, :]
        pivot = pivot_row[:, k : k + 1]
        scaled = pivot_row / pivot
        work = jnp.where(row == k, scaled, work - work[:, k : k + 1] * scaled)
    solved = work[:, count : count + 1]
    solved = jnp.where(row[:, :1] < count, solved, 0.0)
    first = count * (count + 1) // 2
    energy = line[:, first + count : first + count + 1]
    mean_square = energy - jnp.sum(proj * solved, axis=0, keepdims=True)
    norm = jnp.sqrt(mean_square + EPSILON)
    wide = jnp.broadcast_to(solved, (height, 128))
    as_row = jnp.sum(jnp.where(lane == row, wide, 0.0), axis=0, keepdims=True)
    as_row = jnp.where(lane[:1] == count, norm, as_row)
    column[...] = as_row[:, : count + 1]
    weights[...] = wide
    inverse = jnp.broadcast_to(1.0 / norm, (8, 128))

    @pl.loop(0, rows // 8)
    def _(block):
        part = pl.ds(pl.multiple_of(block * 8, 8), 8)
        hess = [jnp.broadcast_to(weights[a : a + 1, :], (8, 128)) for a in range(count)]
        for chunk in range(nodes // 128):
            lanes = slice(chunk * 128, (chunk + 1) * 128)
            terms = [hess[a] * basis[a, part, lanes] for a in range(count)]
            while len(terms) > 1:
                terms = [sum(terms[i : i + 2]) for i in range(0, len(terms), 2)]
            residual[part, lanes] = (product[part, lanes] - terms[0]) * inverse


def in_hbm(value):
    return pltpu.with_memory_space_constraint(value, pltpu.HBM)


def local(
    basis,
    coeffs,
    conductance_tiles,
    tile_cols,
    self_cond,
    cap,
    send_nodes,
    send_count,
    nl_nodes,
    nl_count,
    op_wave,
    nl_gain,
):
    count, _, harm_local, nodes = basis.shape
    rows = 2 * harm_local
    peers = lax.axis_size(DOM)
    groups = lax.axis_size(HARM_AXES)
    peer_cap = send_nodes.shape[2]
    nl_cap = nl_nodes.shape[1]
    basis = basis.reshape(count, rows, nodes)
    smem = pl.BlockSpec(memory_space=pltpu.SMEM)
    vmem = pl.BlockSpec(memory_space=pltpu.VMEM)
    hbm = pl.BlockSpec(memory_space=pl.ANY)
    shape = jax.ShapeDtypeStruct
    params = pltpu.CompilerParams(vmem_limit_bytes=24 * 2**20)
    basis_bytes = 4 * count * rows * nodes

    def cost(flops, size):
        return pl.CostEstimate(flops=flops, bytes_accessed=size, transcendentals=0)

    vector, *ghosts, sampled, cross = pl.pallas_call(
        vector_kernel,
        out_shape=[shape((rows, nodes), F32)]
        + [shape((rows, peer_cap), F32)] * len(PEERS)
        + [shape((groups, harm_local, 128), F32)]
        + [shape((count * 16, count * 8), F32)],
        in_specs=[smem, smem, smem, vmem, vmem, hbm],
        out_specs=[vmem] * (3 + len(PEERS)),
        scratch_shapes=[
            pltpu.VMEM((count, rows, nodes), F32),
            pltpu.VMEM((nodes, len(PEERS) * peer_cap + nl_cap), BF16),
            pltpu.SemaphoreType.DMA((rows // 8,)),
        ],
        compiler_params=params,
        cost_estimate=cost(10**9, basis_bytes),
        name="vector",
    )(
        in_hbm(coeffs), in_hbm(send_count[0]), nl_count,
        in_hbm(send_nodes[0]), in_hbm(nl_nodes), in_hbm(basis),
    )

    arrived_spectrum = lax.all_to_all(sampled, HARM_AXES, 0, 0, tiled=True)
    ghosts = [
        lax.ppermute(ghost, DOM, [(i, (i + jump) % peers) for i in range(peers)])
        for jump, ghost in zip(PEERS, ghosts)
    ]

    leaving = pl.pallas_call(
        current_kernel,
        out_shape=shape((groups, harm_local, 128), F32),
        in_specs=[vmem] * 4,
        out_specs=vmem,
        compiler_params=params,
        cost_estimate=cost(4 * 10**8, 2 * 10**6),
        name="current",
    )(arrived_spectrum, op_wave.T, nl_gain.reshape(1, -1), jnp.asarray(transform_tables()))

    returned = lax.all_to_all(leaving, HARM_AXES, 0, 0, tiled=True)

    tile_rows, terms = tile_cols.shape
    base = pl.pallas_call(
        coupling_kernel,
        out_shape=shape((rows, nodes), F32),
        in_specs=[smem] + [vmem] * (3 + len(PEERS)) + [hbm],
        out_specs=vmem,
        scratch_shapes=[
            pltpu.VMEM((nodes // 128 + peers, 2 * rows, 128), BF16),
            pltpu.VMEM(conductance_tiles.shape, F32),
            pltpu.SemaphoreType.DMA((tile_rows,)),
        ],
        compiler_params=params,
        cost_estimate=cost(10**9, 4 * tile_rows * terms * 128 * 128),
        name="coupling",
    )(
        tile_cols.T, vector, *ghosts, self_cond.reshape(1, -1), cap.reshape(1, -1),
        in_hbm(conductance_tiles),
    )

    devices = peers * groups
    width = 256
    mask, place = unpack_tables(count, 24, width)
    mask, place = jnp.asarray(mask), jnp.asarray(place)
    product, packed, held = pl.pallas_call(
        product_kernel,
        out_shape=[
            shape((rows, nodes), F32),
            shape((devices, width // 128, 128), F32),
            pltpu.VMEM((count, rows, nodes), F32),
        ],
        in_specs=[smem] + [vmem] * 6 + [hbm],
        out_specs=[vmem] * 3,
        scratch_shapes=[
            pltpu.VMEM((width, 128), F32),
            pltpu.SemaphoreType.DMA((rows // 8,)),
        ],
        compiler_params=params,
        cost_estimate=cost(10**9, basis_bytes),
        name="product",
    )(nl_count, nl_nodes, returned, base, cross, mask, place, in_hbm(basis))

    gathered = lax.all_to_all(packed, DOM_HARM, 0, 0, tiled=True)

    entries = rows * groups * nodes * peers
    residual, column = pl.pallas_call(
        functools.partial(residual_kernel, float(entries)),
        out_shape=[shape((rows, nodes), F32), shape((1, count + 1), F32)],
        in_specs=[vmem] * 5,
        out_specs=[vmem, vmem],
        scratch_shapes=[pltpu.VMEM((24, 128), F32)],
        compiler_params=params,
        cost_estimate=cost(10**9, basis_bytes),
        name="residual",
    )(
        gathered, mask, place, product, pltpu.with_memory_space_constraint(held, pltpu.VMEM)
    )
    return (residual.reshape(2, harm_local, nodes), column.reshape(count + 1))


def solution(mesh):
    split = Mesh(mesh.devices.reshape(4, 4, 4, 2), ("dom_0", "dom_1", "harm_0", "harm_1"))
    return jax.shard_map(
        local,
        mesh=split,
        in_specs=(
            P(None, None, HARM_AXES, DOM),
            P(),
            P(DOM, None, None, None),
            P(DOM, None),
            P(DOM),
            P(DOM),
            P(DOM, None, None),
            P(DOM, None),
            P(DOM, None),
            P(DOM),
            P(None, DOM_HARM),
            P(DOM_HARM),
        ),
        out_specs=(P(None, HARM_AXES, DOM), P()),
        check_vma=False,
    )
```

```python
import functools
import math

import ml_dtypes
import numpy as np

import jax
import jax.numpy as jnp
from jax import lax
from jax.experimental import pallas as pl
from jax.experimental.pallas import tpu as pltpu
from jax.sharding import Mesh
from jax.sharding import PartitionSpec as P

HARM = 256
SAMPLES = 2 * HARM
DOM = ("dom_0", "dom_1")
HARM_AXES = ("harm_0", "harm_1")
DOM_HARM = ("dom_0", "dom_1", "harm_0", "harm_1")
PEERS = (1, 15, 8, 9)
EPSILON = 1e-06

F32 = jnp.float32
BF16 = jnp.bfloat16


def halves(value):
    high = value.astype(BF16)
    return high, (value - high.astype(F32)).astype(BF16)


def thirds(value):
    high = value.astype(BF16)
    rest = value - high.astype(F32)
    middle = rest.astype(BF16)
    return high, middle, (rest - middle.astype(F32)).astype(BF16)


def mm(left, right):
    return jnp.dot(left, right, preferred_element_type=F32)


def mm_nt(left, right):
    return lax.dot_general(left, right, (((1,), (1,)), ((), ())), preferred_element_type=F32)


def split_table(table):
    high = table.astype(ml_dtypes.bfloat16)
    low = (table - high.astype(np.float64)).astype(ml_dtypes.bfloat16)
    return [high, low]


def transform_tables():
    index = np.arange(HARM)
    angle = 2.0 * np.pi * ((index[:, None] * index[None, :]) % SAMPLES) / SAMPLES
    cosine, sine = np.cos(angle), np.sin(angle)
    sine[:, 0] = 1.0 - 2.0 * (index % 2)
    return np.stack(split_table(cosine) + split_table(sine) + split_table(sine.T))


def pair_list(count):
    return [(i, j) for i in range(count) for j in range(i, count)]


def unpack_tables(count, rows, width):
    pairs = pair_list(count)
    mask = np.zeros((2, rows, width), np.float32)
    place = np.zeros((2, width, 128), np.float32)
    for position, (i, j) in enumerate(pairs):
        mask[0, i, position] = 1.0
        place[0, position, j] = 1.0
        if i != j:
            mask[1, j, position] = 1.0
            place[1, position, i] = 1.0
    for i in range(count):
        mask[0, i, len(pairs) + i] = 1.0
        place[0, len(pairs) + i, count] = 1.0
    return mask, place.astype(ml_dtypes.bfloat16)


def basis_copy(source, target, sems, block):
    rows = pl.ds(pl.multiple_of(block * 8, 8), 8)
    return pltpu.make_async_copy(source.at[:, rows, :], target.at[:, rows, :], sems.at[block])


def start_all(source, target, sems):
    for block in range(target.shape[1] // 8):
        basis_copy(source, target, sems, block).start()


def row_total(rows_ref):
    ones = jnp.ones((8, rows_ref.shape[1]), BF16)
    return sum(mm_nt(ones, part) for part in thirds(rows_ref[...]))


def vector_kernel(coeffs, send_count, nl_count, send_nodes, nl_nodes, basis_hbm,
                  vector, ghost_0, ghost_1, ghost_2, ghost_3, sampled, cross,
                  basis, select, sems):
    start_all(basis_hbm, basis, sems)
    count, rows, nodes = basis.shape
    peers = send_nodes.shape[0]
    slots = nl_nodes.shape[1]
    cap = send_nodes.shape[1]
    me = lax.axis_index(DOM)
    lane = lax.broadcasted_iota(jnp.int32, (1, cap), 1)
    wanted = []
    for step in PEERS:
        peer = lax.rem(me + step, peers)
        listed = send_nodes[pl.ds(peer, 1), :]
        wanted.append(jnp.where(lane < send_count[peer], listed, -1))
    slot = lax.broadcasted_iota(jnp.int32, (1, slots), 1)
    wanted.append(jnp.where(slot < nl_count[...], nl_nodes[...], -1))
    columns = jnp.concatenate(wanted, axis=1)
    cross[...] = jnp.zeros_like(cross)

    @pl.loop(0, nodes // 128)
    def _(block):
        start = pl.multiple_of(block * 128, 128)
        node = lax.broadcasted_iota(jnp.int32, (128, columns.shape[1]), 0) + start
        select[pl.ds(start, 128), :] = jnp.where(node == columns, 1.0, 0.0).astype(BF16)

    @pl.loop(0, rows // 8)
    def _(block):
        basis_copy(basis_hbm, basis, sems, block).wait()
        part = pl.ds(pl.multiple_of(block * 8, 8), 8)
        total = coeffs[0] * basis[0, part, :]
        for j in range(1, count):
            total = total + coeffs[j] * basis[j, part, :]
        vector[part, :] = total
        both = halves(basis[:, part, :].reshape(count * 8, nodes))
        cross[...] += mm_nt(jnp.concatenate(both, axis=0), both[0])

    left = jnp.concatenate(halves(vector[...]), axis=0)
    half = rows // 2
    low_lanes = lax.broadcasted_iota(jnp.int32, (half, 128), 1) < 64
    ghosts = (ghost_0, ghost_1, ghost_2, ghost_3)
    for start in range(0, columns.shape[1], 256):
        both = mm(left, select[:, start : start + 256])
        both = both[:rows] + both[rows:]
        for item, taken in enumerate((both[:, :128], both[:, 128:])):
            item += start // 128
            if item < len(PEERS):
                ghosts[item][...] = taken
                continue
            pair = item - len(PEERS)
            top, bottom = taken[:half], taken[half:]
            sampled[2 * pair] = jnp.where(low_lanes, top, pltpu.roll(bottom, 64, 1))
            sampled[2 * pair + 1] = jnp.where(low_lanes, pltpu.roll(top, 64, 1), bottom)


def gram_line(cross, mask, place):
    size = cross.shape[1]
    row = lax.broadcasted_iota(jnp.int32, (size, size), 0)
    column = lax.broadcasted_iota(jnp.int32, (size, size), 1)
    matching = row % 8 == column % 8
    first = jnp.where(matching, cross[:size] + cross[size:], 0.0)
    second = jnp.where(matching, cross[size:], 0.0)
    vector = lax.broadcasted_iota(jnp.int32, (128, size), 0)
    owner = lax.broadcasted_iota(jnp.int32, (128, size), 1) // 8
    select = jnp.where(vector == owner, 1.0, 0.0).astype(BF16)
    first = sum(mm(select, part) for part in thirds(first))
    second = sum(mm(select, part) for part in thirds(second))
    gram = sum(mm_nt(part, select) for part in thirds(first))
    gram = gram + sum(mm_nt(select, part) for part in thirds(second))
    height = mask.shape[1]
    spread = sum(mm_nt(part, place[0]) for part in thirds(gram[:height]))
    return jnp.sum(mask[0] * spread, axis=0, keepdims=True)


def current_kernel(arrived, wave, gain, tables, leaving):
    half = HARM // 2
    spectrum = arrived[...].reshape(HARM, 128)
    lane = lax.broadcasted_iota(jnp.int32, (HARM, 128), 1)
    harmonic = lax.broadcasted_iota(jnp.int32, (HARM, 128), 0)
    low = lane < 64
    sign = jnp.where(harmonic % 2 == 0, 1.0, -1.0)
    swapped = pltpu.roll(spectrum, 64, 1)
    even = jnp.where(low, spectrum, swapped * sign)
    odd = jnp.where(low, swapped, spectrum * sign)

    def product(index, values):
        high, lower = values
        return (
            mm(tables[index], high) + mm(tables[index], lower) + mm(tables[index + 1], high)
        )

    waveform = product(0, halves(even)) + product(2, halves(odd))
    gains = jnp.concatenate([gain[...], gain[...]], axis=1)
    growth = jnp.exp(jnp.concatenate([wave[:, :HARM], wave[:, HARM:]], axis=0).T)
    current = halves(gains * growth * waveform)
    weight = jnp.where(harmonic == 0, 1.0 / SAMPLES, 2.0 / SAMPLES)
    cosine = product(0, current)
    sine = product(4, current)
    result = weight * jnp.where(
        low,
        cosine + sign * pltpu.roll(cosine, 64, 1),
        sign * sine + pltpu.roll(sine, 64, 1),
    )
    leaving[...] = result.reshape(leaving.shape)


def coupling_kernel(tile_cols, vector, ghost_0, ghost_1, ghost_2, ghost_3,
                    self_cond, cap, cross, mask, place, tiles_hbm, base, packed_gram,
                    extended, tiles, live, order, sems):
    tile_rows, terms = tiles.shape[:2]

    def tile_copy(row):
        return pltpu.make_async_copy(tiles_hbm.at[row], tiles.at[row], sems.at[row])

    for row in range(tile_rows):
        tile_copy(row).start()
    rows, nodes = vector.shape
    half = rows // 2
    local_tiles = nodes // 128
    peers = extended.shape[0] - local_tiles
    me = lax.axis_index(DOM)
    for tile in range(local_tiles):
        high, low = halves(vector[:, tile * 128 : (tile + 1) * 128])
        extended[tile, :rows] = high
        extended[tile, rows:] = low
    extended[local_tiles:] = jnp.zeros((peers, 2 * rows, 128), BF16)
    for tile in range(local_tiles + peers):
        live[tile] = jnp.int32(tile < local_tiles)
    for jump, ghost in zip(PEERS, (ghost_0, ghost_1, ghost_2, ghost_3)):
        sender = local_tiles + lax.rem(me + peers - jump, peers)
        live[sender] = jnp.int32(1)
        high, low = halves(ghost[...])
        extended[sender, :rows] = high
        extended[sender, rows:] = low

    first = lax.axis_index(HARM_AXES) * half
    harmonic = first + lax.broadcasted_iota(jnp.int32, (half, 128), 0)
    angular = (2.0 * math.pi / HARM) * harmonic.astype(F32)

    packed_gram[...] = gram_line(cross, mask, place)

    def live_first(row, slot):
        flags = [live[tile_cols[i, row]] for i in range(terms)]
        front, back = jnp.int32(0), sum(flags)
        number = back
        for i, flag in enumerate(flags):
            order[slot, jnp.where(flag == 1, front, back)] = jnp.int32(i)
            front, back = front + flag, back + 1 - flag
        return number

    def one_row(row, slot, width):
        picks = [order[slot, i] for i in range(width)]
        left = jnp.concatenate([extended[tile_cols[i, row]] for i in picks], axis=1)
        right = jnp.concatenate([tiles[row, i] for i in picks], axis=0)
        total = mm(left, jnp.concatenate(halves(right), axis=1))
        total = total[:rows, :128] + total[rows:, :128] + total[:rows, 128:]
        lanes = pl.ds(pl.multiple_of(row * 128, 128), 128)
        cosine, sine = vector[:half, lanes], vector[half:, lanes]
        ground, reactive = self_cond[:, lanes], angular * cap[:, lanes]
        base[:half, lanes] = total[:half] + ground * cosine - reactive * sine
        base[half:, lanes] = total[half:] + ground * sine + reactive * cosine

    together = 2

    @pl.loop(0, tile_rows, step=together)
    def _(first_row):
        needed = jnp.int32(0)
        for slot in range(together):
            tile_copy(first_row + slot).wait()
            needed = jnp.maximum(needed, live_first(first_row + slot, slot))
        for width in range(2, terms + 1, 2):
            fits = needed <= width if width < terms else needed >= 0

            @pl.when(fits & (needed > width - 2) if width > 2 else fits)
            def _(width=width):
                for slot in range(together):
                    one_row(first_row + slot, slot, width)


def product_kernel(nl_count, nl_nodes, arrived, base, packed_gram, basis_hbm,
                   product, packed, basis, totals, sems):
    start_all(basis_hbm, basis, sems)
    count, rows, nodes = basis.shape
    half = rows // 2
    slots = nl_nodes.shape[1]
    slot = lax.broadcasted_iota(jnp.int32, (1, slots), 1)
    columns = jnp.where(slot < nl_count[...], nl_nodes[...], -1)
    low_lanes = lax.broadcasted_iota(jnp.int32, (half, 128), 1) < 64
    top, bottom = [], []
    for pair in range(slots // 128):
        even, odd = arrived[2 * pair], arrived[2 * pair + 1]
        top.append(jnp.where(low_lanes, even, pltpu.roll(odd, 64, 1)))
        bottom.append(jnp.where(low_lanes, pltpu.roll(even, 64, 1), odd))
    returned = jnp.concatenate(
        [jnp.concatenate(top, axis=1), jnp.concatenate(bottom, axis=1)], axis=0
    )
    left = jnp.concatenate(halves(returned), axis=0)
    width = 256
    for start in range(0, nodes, width):
        node = lax.broadcasted_iota(jnp.int32, (width, slots), 0) + start
        chosen = jnp.where(node == columns, 1.0, 0.0).astype(BF16)
        added = mm_nt(left, chosen)
        lanes = slice(start, start + width)
        product[:, lanes] = base[:, lanes] + added[:rows] + added[rows:]

    def block_sums(block, sums):
        basis_copy(basis_hbm, basis, sems, block).wait()
        part = pl.ds(pl.multiple_of(block * 8, 8), 8)
        sums = list(sums)
        for chunk in range(nodes // 128):
            lanes = slice(chunk * 128, (chunk + 1) * 128)
            value = product[part, lanes]
            for a in range(count):
                sums[a] = sums[a] + basis[a, part, lanes] * value
            sums[count] = sums[count] + value * value
        return tuple(sums)

    sums = lax.fori_loop(
        0, rows // 8, block_sums, tuple(jnp.zeros((8, 128), F32) for _ in range(count + 1))
    )
    totals[...] = jnp.zeros_like(totals)
    first = count * (count + 1) // 2
    for a in range(count + 1):
        totals[first + a : first + a + 1, :] = jnp.sum(sums[a], axis=0, keepdims=True)
    line = row_total(totals)[:1] + packed_gram[...]
    both = jnp.concatenate([line[:, :128], line[:, 128:]], axis=0)
    packed[...] = jnp.broadcast_to(both[None], packed.shape)


def residual_kernel(entries, gathered, mask, place, product, basis,
                    residual, column, weights):
    count, rows, nodes = basis.shape
    height = mask.shape[1]
    scale = 1.0 / entries
    summed = jnp.sum(gathered[...], axis=0) * scale
    line = jnp.concatenate([summed[:1], summed[1:]], axis=1)
    system = jnp.zeros((height, 128), F32)
    for side in range(2):
        spread = mask[side] * line
        for part in thirds(spread):
            system = system + mm(part, place[side])
    lane = lax.broadcasted_iota(jnp.int32, (height, 128), 1)
    row = lax.broadcasted_iota(jnp.int32, (height, 128), 0)
    proj = jnp.sum(jnp.where(lane == count, system, 0.0), axis=1, keepdims=True)
    work = system
    for k in range(count):
        pivot_row = work[k : k + 1, :]
        pivot = pivot_row[:, k : k + 1]
        scaled = pivot_row / pivot
        work = jnp.where(row == k, scaled, work - work[:, k : k + 1] * scaled)
    solved = work[:, count : count + 1]
    solved = jnp.where(row[:, :1] < count, solved, 0.0)
    first = count * (count + 1) // 2
    energy = line[:, first + count : first + count + 1]
    mean_square = energy - jnp.sum(proj * solved, axis=0, keepdims=True)
    norm = jnp.sqrt(mean_square + EPSILON)
    wide = jnp.broadcast_to(solved, (height, 128))
    as_row = jnp.sum(jnp.where(lane == row, wide, 0.0), axis=0, keepdims=True)
    as_row = jnp.where(lane[:1] == count, norm, as_row)
    column[...] = as_row[:, : count + 1]
    weights[...] = wide
    inverse = jnp.broadcast_to(1.0 / norm, (8, 128))

    @pl.loop(0, rows // 8)
    def _(block):
        part = pl.ds(pl.multiple_of(block * 8, 8), 8)
        hess = [jnp.broadcast_to(weights[a : a + 1, :], (8, 128)) for a in range(count)]
        for chunk in range(nodes // 128):
            lanes = slice(chunk * 128, (chunk + 1) * 128)
            terms = [hess[a] * basis[a, part, lanes] for a in range(count)]
            while len(terms) > 1:
                terms = [sum(terms[i : i + 2]) for i in range(0, len(terms), 2)]
            residual[part, lanes] = (product[part, lanes] - terms[0]) * inverse


def in_hbm(value):
    return pltpu.with_memory_space_constraint(value, pltpu.HBM)


def local(
    basis,
    coeffs,
    conductance_tiles,
    tile_cols,
    self_cond,
    cap,
    send_nodes,
    send_count,
    nl_nodes,
    nl_count,
    op_wave,
    nl_gain,
):
    count, _, harm_local, nodes = basis.shape
    rows = 2 * harm_local
    peers = lax.axis_size(DOM)
    groups = lax.axis_size(HARM_AXES)
    peer_cap = send_nodes.shape[2]
    nl_cap = nl_nodes.shape[1]
    basis = basis.reshape(count, rows, nodes)
    smem = pl.BlockSpec(memory_space=pltpu.SMEM)
    vmem = pl.BlockSpec(memory_space=pltpu.VMEM)
    hbm = pl.BlockSpec(memory_space=pl.ANY)
    shape = jax.ShapeDtypeStruct
    params = pltpu.CompilerParams(vmem_limit_bytes=24 * 2**20)
    basis_bytes = 4 * count * rows * nodes

    def cost(flops, size):
        return pl.CostEstimate(flops=flops, bytes_accessed=size, transcendentals=0)

    vector, *ghosts, sampled, cross = pl.pallas_call(
        vector_kernel,
        out_shape=[shape((rows, nodes), F32)]
        + [shape((rows, peer_cap), F32)] * len(PEERS)
        + [shape((groups, harm_local, 128), F32)]
        + [shape((count * 16, count * 8), F32)],
        in_specs=[smem, smem, vmem, vmem, vmem, hbm],
        out_specs=[vmem] * (3 + len(PEERS)),
        scratch_shapes=[
            pltpu.VMEM((count, rows, nodes), F32),
            pltpu.VMEM((nodes, len(PEERS) * peer_cap + nl_cap), BF16),
            pltpu.SemaphoreType.DMA((rows // 8,)),
        ],
        compiler_params=params,
        cost_estimate=cost(10**9, basis_bytes),
        name="vector",
    )(
        in_hbm(coeffs), in_hbm(send_count[0]), nl_count.reshape(1, 1),
        in_hbm(send_nodes[0]), in_hbm(nl_nodes), in_hbm(basis),
    )

    arrived_spectrum = lax.all_to_all(sampled, HARM_AXES, 0, 0, tiled=True)
    ghosts = [
        lax.ppermute(ghost, DOM, [(i, (i + jump) % peers) for i in range(peers)])
        for jump, ghost in zip(PEERS, ghosts)
    ]

    leaving = pl.pallas_call(
        current_kernel,
        out_shape=shape((groups, harm_local, 128), F32),
        in_specs=[vmem] * 4,
        out_specs=vmem,
        compiler_params=params,
        cost_estimate=cost(4 * 10**8, 2 * 10**6),
        name="current",
    )(arrived_spectrum, op_wave.T, nl_gain.reshape(1, -1), jnp.asarray(transform_tables()))

    returned = lax.all_to_all(leaving, HARM_AXES, 0, 0, tiled=True)

    tile_rows, terms = tile_cols.shape
    width = 256
    mask, place = unpack_tables(count, 24, width)
    mask, place = jnp.asarray(mask), jnp.asarray(place)
    base, packed_gram = pl.pallas_call(
        coupling_kernel,
        out_shape=[shape((rows, nodes), F32), shape((1, width), F32)],
        in_specs=[smem] + [vmem] * (6 + len(PEERS)) + [hbm],
        out_specs=[vmem] * 2,
        scratch_shapes=[
            pltpu.VMEM((nodes // 128 + peers, 2 * rows, 128), BF16),
            pltpu.VMEM(conductance_tiles.shape, F32),
            pltpu.SMEM((nodes // 128 + peers,), jnp.int32),
            pltpu.SMEM((2, terms), jnp.int32),
            pltpu.SemaphoreType.DMA((tile_rows,)),
        ],
        compiler_params=params,
        cost_estimate=cost(10**9, 4 * tile_rows * terms * 128 * 128),
        name="coupling",
    )(
        tile_cols.T, vector, *ghosts, self_cond.reshape(1, -1), cap.reshape(1, -1),
        cross, mask, place, in_hbm(conductance_tiles),
    )

    devices = peers * groups
    product, packed, held = pl.pallas_call(
        product_kernel,
        out_shape=[
            shape((rows, nodes), F32),
            shape((devices, width // 128, 128), F32),
            pltpu.VMEM((count, rows, nodes), F32),
        ],
        in_specs=[vmem] * 5 + [hbm],
        out_specs=[vmem] * 3,
        scratch_shapes=[
            pltpu.VMEM((width, 128), F32),
            pltpu.SemaphoreType.DMA((rows // 8,)),
        ],
        compiler_params=params,
        cost_estimate=cost(10**9, basis_bytes),
        name="product",
    )(nl_count.reshape(1, 1), nl_nodes, returned, base, packed_gram, in_hbm(basis))

    gathered = lax.all_to_all(packed, DOM_HARM, 0, 0, tiled=True)

    entries = rows * groups * nodes * peers
    residual, column = pl.pallas_call(
        functools.partial(residual_kernel, float(entries)),
        out_shape=[shape((rows, nodes), F32), shape((1, count + 1), F32)],
        in_specs=[vmem] * 5,
        out_specs=[vmem, vmem],
        scratch_shapes=[pltpu.VMEM((24, 128), F32)],
        compiler_params=params,
        cost_estimate=cost(10**9, basis_bytes),
        name="residual",
    )(
        gathered, mask, place, product, pltpu.with_memory_space_constraint(held, pltpu.VMEM)
    )
    return (residual.reshape(2, harm_local, nodes), column.reshape(count + 1))


def solution(mesh):
    split = Mesh(mesh.devices.reshape(4, 4, 4, 2), ("dom_0", "dom_1", "harm_0", "harm_1"))
    return jax.shard_map(
        local,
        mesh=split,
        in_specs=(
            P(None, None, HARM_AXES, DOM),
            P(),
            P(DOM, None, None, None),
            P(DOM, None),
            P(DOM),
            P(DOM),
            P(DOM, None, None),
            P(DOM, None),
            P(DOM, None),
            P(DOM),
            P(None, DOM_HARM),
            P(DOM_HARM),
        ),
        out_specs=(P(None, HARM_AXES, DOM), P()),
        check_vma=False,
    )
```

```python
import functools
import math

import ml_dtypes
import numpy as np

import jax
import jax.numpy as jnp
from jax import lax
from jax.experimental import pallas as pl
from jax.experimental.pallas import tpu as pltpu
from jax.sharding import Mesh
from jax.sharding import PartitionSpec as P

HARM = 256
SAMPLES = 2 * HARM
DOM = ("dom_0", "dom_1")
HARM_AXES = ("harm_0", "harm_1")
DOM_HARM = ("dom_0", "dom_1", "harm_0", "harm_1")
PEERS = (1, 15, 8, 9)
EPSILON = 1e-06

F32 = jnp.float32
BF16 = jnp.bfloat16


def halves(value):
    high = value.astype(BF16)
    return high, (value - high.astype(F32)).astype(BF16)


def thirds(value):
    high = value.astype(BF16)
    rest = value - high.astype(F32)
    middle = rest.astype(BF16)
    return high, middle, (rest - middle.astype(F32)).astype(BF16)


def mm(left, right):
    return jnp.dot(left, right, preferred_element_type=F32)


def mm_nt(left, right):
    return lax.dot_general(left, right, (((1,), (1,)), ((), ())), preferred_element_type=F32)


def split_table(table):
    high = table.astype(ml_dtypes.bfloat16)
    low = (table - high.astype(np.float64)).astype(ml_dtypes.bfloat16)
    return [high, low]


def transform_tables():
    index = np.arange(HARM)
    angle = 2.0 * np.pi * ((index[:, None] * index[None, :]) % SAMPLES) / SAMPLES
    cosine, sine = np.cos(angle), np.sin(angle)
    sine[:, 0] = 1.0 - 2.0 * (index % 2)
    return np.stack(split_table(cosine) + split_table(sine) + split_table(sine.T))


def pair_list(count):
    return [(i, j) for i in range(count) for j in range(i, count)]


def unpack_tables(count, rows, width):
    pairs = pair_list(count)
    mask = np.zeros((2, rows, width), np.float32)
    place = np.zeros((2, width, 128), np.float32)
    for position, (i, j) in enumerate(pairs):
        mask[0, i, position] = 1.0
        place[0, position, j] = 1.0
        if i != j:
            mask[1, j, position] = 1.0
            place[1, position, i] = 1.0
    for i in range(count):
        mask[0, i, len(pairs) + i] = 1.0
        place[0, len(pairs) + i, count] = 1.0
    return mask, place.astype(ml_dtypes.bfloat16)


def basis_copy(source, target, sems, block):
    rows = pl.ds(pl.multiple_of(block * 8, 8), 8)
    return pltpu.make_async_copy(source.at[:, rows, :], target.at[:, rows, :], sems.at[block])


def start_all(source, target, sems):
    for block in range(target.shape[1] // 8):
        basis_copy(source, target, sems, block).start()


def row_total(rows_ref):
    ones = jnp.ones((8, rows_ref.shape[1]), BF16)
    return sum(mm_nt(ones, part) for part in thirds(rows_ref[...]))


def vector_kernel(coeffs, send_count, send_nodes, nl_nodes, basis_hbm,
                  vector, ghost_0, ghost_1, ghost_2, ghost_3, sampled, cross,
                  basis, select, sems):
    start_all(basis_hbm, basis, sems)
    count, rows, nodes = basis.shape
    peers = send_nodes.shape[0]
    slots = nl_nodes.shape[1]
    cap = send_nodes.shape[1]
    me = lax.axis_index(DOM)
    lane = lax.broadcasted_iota(jnp.int32, (1, cap), 1)
    wanted = []
    for step in PEERS:
        peer = lax.rem(me + step, peers)
        listed = send_nodes[pl.ds(peer, 1), :]
        wanted.append(jnp.where(lane < send_count[peer], listed, -1))
    wanted.append(nl_nodes[...])
    columns = jnp.concatenate(wanted, axis=1)
    cross[...] = jnp.zeros_like(cross)

    @pl.loop(0, nodes // 128)
    def _(block):
        start = pl.multiple_of(block * 128, 128)
        node = lax.broadcasted_iota(jnp.int32, (128, columns.shape[1]), 0) + start
        select[pl.ds(start, 128), :] = jnp.where(node == columns, 1.0, 0.0).astype(BF16)

    @pl.loop(0, rows // 8)
    def _(block):
        basis_copy(basis_hbm, basis, sems, block).wait()
        part = pl.ds(pl.multiple_of(block * 8, 8), 8)
        total = coeffs[0] * basis[0, part, :]
        for j in range(1, count):
            total = total + coeffs[j] * basis[j, part, :]
        vector[part, :] = total
        both = halves(basis[:, part, :].reshape(count * 8, nodes))
        cross[...] += mm_nt(jnp.concatenate(both, axis=0), both[0])

    left = jnp.concatenate(halves(vector[...]), axis=0)
    half = rows // 2
    low_lanes = lax.broadcasted_iota(jnp.int32, (half, 128), 1) < 64
    ghosts = (ghost_0, ghost_1, ghost_2, ghost_3)
    for start in range(0, columns.shape[1], 256):
        both = mm(left, select[:, start : start + 256])
        both = both[:rows] + both[rows:]
        for item, taken in enumerate((both[:, :128], both[:, 128:])):
            item += start // 128
            if item < len(PEERS):
                ghosts[item][...] = taken
                continue
            pair = item - len(PEERS)
            top, bottom = taken[:half], taken[half:]
            sampled[2 * pair] = jnp.where(low_lanes, top, pltpu.roll(bottom, 64, 1))
            sampled[2 * pair + 1] = jnp.where(low_lanes, pltpu.roll(top, 64, 1), bottom)


def gram_line(cross, mask, place):
    size = cross.shape[1]
    row = lax.broadcasted_iota(jnp.int32, (size, size), 0)
    column = lax.broadcasted_iota(jnp.int32, (size, size), 1)
    matching = row % 8 == column % 8
    first = jnp.where(matching, cross[:size] + cross[size:], 0.0)
    second = jnp.where(matching, cross[size:], 0.0)
    vector = lax.broadcasted_iota(jnp.int32, (128, size), 0)
    owner = lax.broadcasted_iota(jnp.int32, (128, size), 1) // 8
    select = jnp.where(vector == owner, 1.0, 0.0).astype(BF16)
    first = sum(mm(select, part) for part in thirds(first))
    second = sum(mm(select, part) for part in thirds(second))
    gram = sum(mm_nt(part, select) for part in thirds(first))
    gram = gram + sum(mm_nt(select, part) for part in thirds(second))
    height = mask.shape[1]
    spread = sum(mm_nt(part, place[0]) for part in thirds(gram[:height]))
    return jnp.sum(mask[0] * spread, axis=0, keepdims=True)


def current_kernel(arrived, wave, gain, tables, leaving):
    half = HARM // 2
    spectrum = arrived[...].reshape(HARM, 128)
    lane = lax.broadcasted_iota(jnp.int32, (HARM, 128), 1)
    harmonic = lax.broadcasted_iota(jnp.int32, (HARM, 128), 0)
    low = lane < 64
    sign = jnp.where(harmonic % 2 == 0, 1.0, -1.0)
    swapped = pltpu.roll(spectrum, 64, 1)
    even = jnp.where(low, spectrum, swapped * sign)
    odd = jnp.where(low, swapped, spectrum * sign)

    def product(index, values):
        high, lower = values
        return (
            mm(tables[index], high) + mm(tables[index], lower) + mm(tables[index + 1], high)
        )

    waveform = product(0, halves(even)) + product(2, halves(odd))
    gains = jnp.concatenate([gain[...], gain[...]], axis=1)
    growth = jnp.exp(jnp.concatenate([wave[:, :HARM], wave[:, HARM:]], axis=0).T)
    current = halves(gains * growth * waveform)
    weight = jnp.where(harmonic == 0, 1.0 / SAMPLES, 2.0 / SAMPLES)
    cosine = product(0, current)
    sine = product(4, current)
    result = weight * jnp.where(
        low,
        cosine + sign * pltpu.roll(cosine, 64, 1),
        sign * sine + pltpu.roll(sine, 64, 1),
    )
    leaving[...] = result.reshape(leaving.shape)


def coupling_kernel(tile_cols, vector, ghost_0, ghost_1, ghost_2, ghost_3,
                    self_cond, cap, cross, mask, place, tiles_hbm, base, packed_gram,
                    extended, tiles, live, order, sems):
    tile_rows, terms = tiles.shape[:2]

    def tile_copy(row):
        return pltpu.make_async_copy(tiles_hbm.at[row], tiles.at[row], sems.at[row])

    for row in range(tile_rows):
        tile_copy(row).start()
    rows, nodes = vector.shape
    half = rows // 2
    local_tiles = nodes // 128
    peers = extended.shape[0] - local_tiles
    me = lax.axis_index(DOM)
    for tile in range(local_tiles):
        high, low = halves(vector[:, tile * 128 : (tile + 1) * 128])
        extended[tile, :rows] = high
        extended[tile, rows:] = low
    extended[local_tiles:] = jnp.zeros((peers, 2 * rows, 128), BF16)
    for tile in range(local_tiles + peers):
        live[tile] = jnp.int32(tile < local_tiles)
    for jump, ghost in zip(PEERS, (ghost_0, ghost_1, ghost_2, ghost_3)):
        sender = local_tiles + lax.rem(me + peers - jump, peers)
        live[sender] = jnp.int32(1)
        high, low = halves(ghost[...])
        extended[sender, :rows] = high
        extended[sender, rows:] = low

    first = lax.axis_index(HARM_AXES) * half
    harmonic = first + lax.broadcasted_iota(jnp.int32, (half, 128), 0)
    angular = (2.0 * math.pi / HARM) * harmonic.astype(F32)

    packed_gram[...] = gram_line(cross, mask, place)

    def live_first(row, slot):
        flags = [live[tile_cols[i, row]] for i in range(terms)]
        front, back = jnp.int32(0), sum(flags)
        number = back
        for i, flag in enumerate(flags):
            order[slot, jnp.where(flag == 1, front, back)] = jnp.int32(i)
            front, back = front + flag, back + 1 - flag
        return number

    def one_row(row, slot, width):
        picks = [order[slot, i] for i in range(width)]
        left = jnp.concatenate([extended[tile_cols[i, row]] for i in picks], axis=1)
        right = jnp.concatenate([tiles[row, i] for i in picks], axis=0)
        total = mm(left, jnp.concatenate(halves(right), axis=1))
        total = total[:rows, :128] + total[rows:, :128] + total[:rows, 128:]
        lanes = pl.ds(pl.multiple_of(row * 128, 128), 128)
        cosine, sine = vector[:half, lanes], vector[half:, lanes]
        ground, reactive = self_cond[:, lanes], angular * cap[:, lanes]
        base[:half, lanes] = total[:half] + ground * cosine - reactive * sine
        base[half:, lanes] = total[half:] + ground * sine + reactive * cosine

    together = 2

    @pl.loop(0, tile_rows, step=together)
    def _(first_row):
        needed = jnp.int32(0)
        for slot in range(together):
            tile_copy(first_row + slot).wait()
            needed = jnp.maximum(needed, live_first(first_row + slot, slot))
        for width in range(2, terms + 1, 2):
            fits = needed <= width if width < terms else needed >= 0

            @pl.when(fits & (needed > width - 2) if width > 2 else fits)
            def _(width=width):
                for slot in range(together):
                    one_row(first_row + slot, slot, width)


def product_kernel(nl_count, nl_nodes, arrived, base, packed_gram, basis_hbm,
                   product, packed, basis, totals, sems):
    start_all(basis_hbm, basis, sems)
    count, rows, nodes = basis.shape
    half = rows // 2
    slots = nl_nodes.shape[1]
    slot = lax.broadcasted_iota(jnp.int32, (1, slots), 1)
    columns = jnp.where(slot < nl_count[0], nl_nodes[...], -1)
    low_lanes = lax.broadcasted_iota(jnp.int32, (half, 128), 1) < 64
    top, bottom = [], []
    for pair in range(slots // 128):
        even, odd = arrived[2 * pair], arrived[2 * pair + 1]
        top.append(jnp.where(low_lanes, even, pltpu.roll(odd, 64, 1)))
        bottom.append(jnp.where(low_lanes, pltpu.roll(even, 64, 1), odd))
    returned = jnp.concatenate(
        [jnp.concatenate(top, axis=1), jnp.concatenate(bottom, axis=1)], axis=0
    )
    left = jnp.concatenate(halves(returned), axis=0)
    width = 256
    for start in range(0, nodes, width):
        node = lax.broadcasted_iota(jnp.int32, (width, slots), 0) + start
        chosen = jnp.where(node == columns, 1.0, 0.0).astype(BF16)
        added = mm_nt(left, chosen)
        lanes = slice(start, start + width)
        product[:, lanes] = base[:, lanes] + added[:rows] + added[rows:]

    def block_sums(block, sums):
        basis_copy(basis_hbm, basis, sems, block).wait()
        part = pl.ds(pl.multiple_of(block * 8, 8), 8)
        sums = list(sums)
        for chunk in range(nodes // 128):
            lanes = slice(chunk * 128, (chunk + 1) * 128)
            value = product[part, lanes]
            for a in range(count):
                sums[a] = sums[a] + basis[a, part, lanes] * value
            sums[count] = sums[count] + value * value
        return tuple(sums)

    sums = lax.fori_loop(
        0, rows // 8, block_sums, tuple(jnp.zeros((8, 128), F32) for _ in range(count + 1))
    )
    totals[...] = jnp.zeros_like(totals)
    first = count * (count + 1) // 2
    for a in range(count + 1):
        totals[first + a : first + a + 1, :] = jnp.sum(sums[a], axis=0, keepdims=True)
    line = row_total(totals)[:1] + packed_gram[...]
    both = jnp.concatenate([line[:, :128], line[:, 128:]], axis=0)
    packed[...] = jnp.broadcast_to(both[None], packed.shape)


def residual_kernel(entries, gathered, mask, place, product, basis,
                    residual, column, weights):
    count, rows, nodes = basis.shape
    height = mask.shape[1]
    scale = 1.0 / entries
    summed = jnp.sum(gathered[...], axis=0) * scale
    line = jnp.concatenate([summed[:1], summed[1:]], axis=1)
    system = jnp.zeros((height, 128), F32)
    for side in range(2):
        spread = mask[side] * line
        for part in thirds(spread):
            system = system + mm(part, place[side])
    lane = lax.broadcasted_iota(jnp.int32, (height, 128), 1)
    row = lax.broadcasted_iota(jnp.int32, (height, 128), 0)
    proj = jnp.sum(jnp.where(lane == count, system, 0.0), axis=1, keepdims=True)
    work = system
    for k in range(count):
        pivot_row = work[k : k + 1, :]
        pivot = pivot_row[:, k : k + 1]
        scaled = pivot_row / pivot
        work = jnp.where(row == k, scaled, work - work[:, k : k + 1] * scaled)
    solved = work[:, count : count + 1]
    solved = jnp.where(row[:, :1] < count, solved, 0.0)
    first = count * (count + 1) // 2
    energy = line[:, first + count : first + count + 1]
    mean_square = energy - jnp.sum(proj * solved, axis=0, keepdims=True)
    norm = jnp.sqrt(mean_square + EPSILON)
    wide = jnp.broadcast_to(solved, (height, 128))
    as_row = jnp.sum(jnp.where(lane == row, wide, 0.0), axis=0, keepdims=True)
    as_row = jnp.where(lane[:1] == count, norm, as_row)
    column[...] = as_row[:, : count + 1]
    weights[...] = wide
    inverse = jnp.broadcast_to(1.0 / norm, (8, 128))

    @pl.loop(0, rows // 8)
    def _(block):
        part = pl.ds(pl.multiple_of(block * 8, 8), 8)
        hess = [jnp.broadcast_to(weights[a : a + 1, :], (8, 128)) for a in range(count)]
        for chunk in range(nodes // 128):
            lanes = slice(chunk * 128, (chunk + 1) * 128)
            terms = [hess[a] * basis[a, part, lanes] for a in range(count)]
            while len(terms) > 1:
                terms = [sum(terms[i : i + 2]) for i in range(0, len(terms), 2)]
            residual[part, lanes] = (product[part, lanes] - terms[0]) * inverse


def in_hbm(value):
    return pltpu.with_memory_space_constraint(value, pltpu.HBM)


def local(
    basis,
    coeffs,
    conductance_tiles,
    tile_cols,
    self_cond,
    cap,
    send_nodes,
    send_count,
    nl_nodes,
    nl_count,
    op_wave,
    nl_gain,
):
    count, _, harm_local, nodes = basis.shape
    rows = 2 * harm_local
    peers = lax.axis_size(DOM)
    groups = lax.axis_size(HARM_AXES)
    peer_cap = send_nodes.shape[2]
    nl_cap = nl_nodes.shape[1]
    basis = basis.reshape(count, rows, nodes)
    smem = pl.BlockSpec(memory_space=pltpu.SMEM)
    vmem = pl.BlockSpec(memory_space=pltpu.VMEM)
    hbm = pl.BlockSpec(memory_space=pl.ANY)
    shape = jax.ShapeDtypeStruct
    params = pltpu.CompilerParams(vmem_limit_bytes=24 * 2**20)
    basis_bytes = 4 * count * rows * nodes

    def cost(flops, size):
        return pl.CostEstimate(flops=flops, bytes_accessed=size, transcendentals=0)

    vector, *ghosts, sampled, cross = pl.pallas_call(
        vector_kernel,
        out_shape=[shape((rows, nodes), F32)]
        + [shape((rows, peer_cap), F32)] * len(PEERS)
        + [shape((groups, harm_local, 128), F32)]
        + [shape((count * 16, count * 8), F32)],
        in_specs=[smem, smem, vmem, vmem, hbm],
        out_specs=[vmem] * (3 + len(PEERS)),
        scratch_shapes=[
            pltpu.VMEM((count, rows, nodes), F32),
            pltpu.VMEM((nodes, len(PEERS) * peer_cap + nl_cap), BF16),
            pltpu.SemaphoreType.DMA((rows // 8,)),
        ],
        compiler_params=params,
        cost_estimate=cost(10**9, basis_bytes),
        name="vector",
    )(
        in_hbm(coeffs), in_hbm(send_count[0]),
        in_hbm(send_nodes[0]), in_hbm(nl_nodes), in_hbm(basis),
    )

    arrived_spectrum = lax.all_to_all(sampled, HARM_AXES, 0, 0, tiled=True)
    ghosts = [
        lax.ppermute(ghost, DOM, [(i, (i + jump) % peers) for i in range(peers)])
        for jump, ghost in zip(PEERS, ghosts)
    ]

    leaving = pl.pallas_call(
        current_kernel,
        out_shape=shape((groups, harm_local, 128), F32),
        in_specs=[vmem] * 4,
        out_specs=vmem,
        compiler_params=params,
        cost_estimate=cost(4 * 10**8, 2 * 10**6),
        name="current",
    )(arrived_spectrum, op_wave.T, nl_gain.reshape(1, -1), jnp.asarray(transform_tables()))

    returned = lax.all_to_all(leaving, HARM_AXES, 0, 0, tiled=True)

    tile_rows, terms = tile_cols.shape
    width = 256
    mask, place = unpack_tables(count, 24, width)
    mask, place = jnp.asarray(mask), jnp.asarray(place)
    base, packed_gram = pl.pallas_call(
        coupling_kernel,
        out_shape=[shape((rows, nodes), F32), shape((1, width), F32)],
        in_specs=[smem] + [vmem] * (6 + len(PEERS)) + [hbm],
        out_specs=[vmem] * 2,
        scratch_shapes=[
            pltpu.VMEM((nodes // 128 + peers, 2 * rows, 128), BF16),
            pltpu.VMEM(conductance_tiles.shape, F32),
            pltpu.SMEM((nodes // 128 + peers,), jnp.int32),
            pltpu.SMEM((2, terms), jnp.int32),
            pltpu.SemaphoreType.DMA((tile_rows,)),
        ],
        compiler_params=params,
        cost_estimate=cost(10**9, 4 * tile_rows * terms * 128 * 128),
        name="coupling",
    )(
        tile_cols.T, vector, *ghosts, self_cond.reshape(1, -1), cap.reshape(1, -1),
        cross, mask, place, in_hbm(conductance_tiles),
    )

    devices = peers * groups
    product, packed, held = pl.pallas_call(
        product_kernel,
        out_shape=[
            shape((rows, nodes), F32),
            shape((devices, width // 128, 128), F32),
            pltpu.VMEM((count, rows, nodes), F32),
        ],
        in_specs=[smem] + [vmem] * 4 + [hbm],
        out_specs=[vmem] * 3,
        scratch_shapes=[
            pltpu.VMEM((width, 128), F32),
            pltpu.SemaphoreType.DMA((rows // 8,)),
        ],
        compiler_params=params,
        cost_estimate=cost(10**9, basis_bytes),
        name="product",
    )(nl_count, nl_nodes, returned, base, packed_gram, in_hbm(basis))

    gathered = lax.all_to_all(packed, DOM_HARM, 0, 0, tiled=True)

    entries = rows * groups * nodes * peers
    residual, column = pl.pallas_call(
        functools.partial(residual_kernel, float(entries)),
        out_shape=[shape((rows, nodes), F32), shape((1, count + 1), F32)],
        in_specs=[vmem] * 5,
        out_specs=[vmem, vmem],
        scratch_shapes=[pltpu.VMEM((24, 128), F32)],
        compiler_params=params,
        cost_estimate=cost(10**9, basis_bytes),
        name="residual",
    )(
        gathered, mask, place, product, pltpu.with_memory_space_constraint(held, pltpu.VMEM)
    )
    return (residual.reshape(2, harm_local, nodes), column.reshape(count + 1))


def solution(mesh):
    split = Mesh(mesh.devices.reshape(4, 4, 4, 2), ("dom_0", "dom_1", "harm_0", "harm_1"))
    return jax.shard_map(
        local,
        mesh=split,
        in_specs=(
            P(None, None, HARM_AXES, DOM),
            P(),
            P(DOM, None, None, None),
            P(DOM, None),
            P(DOM),
            P(DOM),
            P(DOM, None, None),
            P(DOM, None),
            P(DOM, None),
            P(DOM),
            P(None, DOM_HARM),
            P(DOM_HARM),
        ),
        out_specs=(P(None, HARM_AXES, DOM), P()),
        check_vma=False,
    )
```
